16 devices in a mesh: data: 16 (over z, y, x, core).
Axes of the slice: x: 2, y: 2, z: 2, core: 2. Of those that a mesh axis runs over, the one named last changes fastest.
Arguments:
- feat_img: bfloat16 [16384, 1152], P('data')
- feat_txt: bfloat16 [16384, 1152], P('data')
- w_img: bfloat16 [1152, 1152], replicated
- w_txt: bfloat16 [1152, 1152], replicated
- log_temp: float32 [], replicated
- logit_bias: float32 [], replicated
- pair_ids: int32 [16384], P('data')
Outputs:
- output 1: float32 [], replicated
- output 2: float32 [], replicated
- output 3: float32 [], replicated
- output 4: float32 [1152, 1152], replicated
- output 5: float32 [1152, 1152], replicated
All inputs are finite; a program needn't handle non-finite values.
Results may differ from the reference program's by a relative error of at most 0.001.
Values are sent between devices in bfloat16 or wider.
A program may use at most 1 GiB of HBM per device.

```python
import jax
import jax.numpy as jnp
from jax import lax

ROWS_DEV = 1024
DEVICES = 16
EMBED = 1152
FEAT_IMG = 1152
FEAT_TXT = 1152
LATENT = 16

BATCH = ROWS_DEV * DEVICES


def feature_draw(base_key, feat_width):
    key_list = jax.random.split(base_key, 4)
    latents = jax.random.normal(key_list[0], (BATCH, LATENT), jnp.float32)
    basis_rows = jax.random.normal(key_list[1], (LATENT, feat_width), jnp.float32)
    center = jax.random.normal(key_list[2], (feat_width,), jnp.float32)
    noise_rows = jax.random.normal(key_list[3], (BATCH, feat_width), jnp.float32)
    feat_out = center + jnp.dot(latents, basis_rows) * LATENT ** -0.5 + 0.5 * noise_rows
    return feat_out.astype(jnp.bfloat16)


def setup_inputs(seed: int = 0) -> dict:
    key_list = jax.random.split(jax.random.key(seed), 7)
    w_img = jax.random.normal(key_list[2], (FEAT_IMG, EMBED), jnp.float32) * FEAT_IMG ** -0.5
    w_txt = jax.random.normal(key_list[3], (FEAT_TXT, EMBED), jnp.float32) * FEAT_TXT ** -0.5
    log_temp = jnp.log(10.0) + jax.random.uniform(key_list[4], (), jnp.float32, -0.5, 0.5)
    logit_bias = -jnp.log(float(BATCH)) + jax.random.uniform(key_list[5], (), jnp.float32, -0.5, 1.5)
    pair_ids = (jax.random.permutation(key_list[6], BATCH) // 2).astype(jnp.int32)
    return {
        "feat_img": feature_draw(key_list[0], FEAT_IMG),
        "feat_txt": feature_draw(key_list[1], FEAT_TXT),
        "w_img": w_img.astype(jnp.bfloat16),
        "w_txt": w_txt.astype(jnp.bfloat16),
        "log_temp": log_temp.astype(jnp.float32),
        "logit_bias": logit_bias.astype(jnp.float32),
        "pair_ids": pair_ids,
    }


def reference(feat_img, feat_txt, w_img, w_txt, log_temp, logit_bias, pair_ids):
    temp_scale = jnp.exp(log_temp)
    raw_img = jnp.dot(feat_img, w_img, preferred_element_type=jnp.float32)
    raw_txt = jnp.dot(feat_txt, w_txt, preferred_element_type=jnp.float32)
    inv_img = lax.rsqrt(jnp.sum(raw_img * raw_img, axis=1, keepdims=True))
    inv_txt = lax.rsqrt(jnp.sum(raw_txt * raw_txt, axis=1, keepdims=True))
    unit_img = raw_img * inv_img
    unit_txt = raw_txt * inv_txt
    emb_img = unit_img.astype(jnp.bfloat16)
    emb_txt = unit_txt.astype(jnp.bfloat16)

    def row_block(loop_state, block_in):
        acc_txt, loss_sum, temp_sum, bias_sum = loop_state
        emb_blk, ids_blk = block_in
        sim_tile = jnp.dot(emb_blk, emb_txt.T, preferred_element_type=jnp.float32)
        label_sign = jnp.where(ids_blk[:, None] == pair_ids[None, :], 1.0, -1.0).astype(jnp.float32)
        margin = -label_sign * (temp_scale * sim_tile + logit_bias)
        grad_tile = -label_sign * jax.nn.sigmoid(margin) / BATCH
        grad_bf = grad_tile.astype(jnp.bfloat16)
        grad_blk = jnp.dot(grad_bf, emb_txt, preferred_element_type=jnp.float32)
        acc_txt = acc_txt + jnp.dot(grad_bf.T, emb_blk, preferred_element_type=jnp.float32)
        new_state = (
            acc_txt,
            loss_sum + jnp.sum(jax.nn.softplus(margin)),
            temp_sum + jnp.sum(grad_tile * sim_tile),
            bias_sum + jnp.sum(grad_tile),
        )
        return new_state, grad_blk

    zero_sum = jnp.zeros((), jnp.float32)
    init_state = (jnp.zeros((BATCH, EMBED), jnp.float32), zero_sum, zero_sum, zero_sum)
    block_in = (emb_img.reshape(DEVICES, ROWS_DEV, EMBED), pair_ids.reshape(DEVICES, ROWS_DEV))
    final_state, grad_blocks = lax.scan(row_block, init_state, block_in)
    acc_txt, loss_sum, temp_sum, bias_sum = final_state
    grad_img = temp_scale * grad_blocks.reshape(BATCH, EMBED)
    grad_txt = temp_scale * acc_txt
    raw_grad_img = inv_img * (grad_img - unit_img * jnp.sum(unit_img * grad_img, axis=1, keepdims=True))
    raw_grad_txt = inv_txt * (grad_txt - unit_txt * jnp.sum(unit_txt * grad_txt, axis=1, keepdims=True))
    grad_w_img = jnp.dot(feat_img.T, raw_grad_img.astype(jnp.bfloat16), preferred_element_type=jnp.float32)
    grad_w_txt = jnp.dot(feat_txt.T, raw_grad_txt.astype(jnp.bfloat16), preferred_element_type=jnp.float32)
    return loss_sum / BATCH, temp_scale * temp_sum, bias_sum, grad_w_img, grad_w_txt
```

```python
import functools

import jax
import jax.numpy as jnp
from jax import lax
from jax.experimental import pallas as pl
from jax.experimental.pallas import tpu as pltpu
from jax.sharding import PartitionSpec as P

CONTRACT_ROWS = (((0,), (0,)), ((), ()))
CONTRACT_COLS = (((1,), (1,)), ((), ()))
LOG2E = 1.4426950408889634


def embed_rows(feat_rows, weights):
    raw_emb = jnp.dot(feat_rows, weights, preferred_element_type=jnp.float32)
    inv_norm = lax.rsqrt(jnp.sum(raw_emb * raw_emb, axis=1, keepdims=True))
    unit_emb = raw_emb * inv_norm
    return unit_emb, inv_norm, unit_emb.astype(jnp.bfloat16)


def weight_grad(feat_rows, unit_emb, inv_norm, grad_emb):
    raw_grad = inv_norm * (grad_emb - unit_emb * jnp.sum(unit_emb * grad_emb, axis=1, keepdims=True))
    return lax.dot_general(feat_rows, raw_grad.astype(jnp.bfloat16), CONTRACT_ROWS, preferred_element_type=jnp.float32)


def pair_kernel(want, first, sub, scal, own, rem, ids_own, ids_rem, *refs):
    n_in = 0 if first else (4 if want else 1)
    prev, outs = refs[:n_in], refs[n_in:]
    acc = outs[0]

    @pl.when(pl.program_id(0) == 0)
    def _():
        for i, out in enumerate(outs):
            out[...] = jnp.zeros_like(out) if first else prev[i][...]

    neg_scale, neg_bias = scal[0], scal[1]
    rem_rows = rem.shape[0]
    n_sub = rem_rows // sub

    def sim(k):
        return lax.dot_general(own[...], rem[k * sub:(k + 1) * sub, :], CONTRACT_COLS, preferred_element_type=jnp.float32)

    def fold(x):
        y = x[:, 0:128]
        for c in range(1, sub // 128):
            y = y + x[:, c * 128:(c + 1) * 128]
        return jnp.sum(y.reshape(-1, 8, 128), axis=0)

    sims = [sim(0)]
    grads = []
    for k in range(n_sub):
        if k + 1 < n_sub:
            sims.append(sim(k + 1))
        pos = ids_own[...] == ids_rem[:, k * sub:(k + 1) * sub]
        neg_y = jnp.where(pos, -1.0, 1.0)
        yz = (sims[k] * neg_scale + neg_bias) * neg_y
        if want:
            e = jnp.exp2(-jnp.abs(yz))
            r = 1.0 / (1.0 + e)
            grad = jnp.where(yz <= 0, r, e * r) * neg_y
            outs[1][...] += fold(jnp.log1p(e)) * LOG2E - fold(jnp.minimum(yz, 0.0))
            outs[2][...] += fold(grad * sims[k])
            outs[3][...] += fold(grad)
        else:
            grad = neg_y / (1.0 + jnp.exp2(yz))
        grads.append(grad.astype(jnp.bfloat16))
    acc[...] += jnp.dot(jnp.concatenate(grads, axis=1) if n_sub > 1 else grads[0], rem[...],
                        preferred_element_type=jnp.float32)


def pair_call(own, rem, ids_own, ids_rem, scal, prev, want, blk, sub):
    rows, dim = own.shape
    n_rem = rem.shape[0]
    first = prev is None
    outs = [jax.ShapeDtypeStruct((rows, dim), jnp.float32)]
    specs = [pl.BlockSpec((rows, dim), lambda j: (0, 0))]
    if want:
        outs += [jax.ShapeDtypeStruct((8, 128), jnp.float32)] * 3
        specs += [pl.BlockSpec((8, 128), lambda j: (0, 0))] * 3
    in_specs = [pl.BlockSpec(memory_space=pltpu.SMEM),
                pl.BlockSpec((rows, dim), lambda j: (0, 0)),
                pl.BlockSpec((blk, dim), lambda j: (j, 0)),
                pl.BlockSpec((rows, 1), lambda j: (0, 0)),
                pl.BlockSpec((1, blk), lambda j: (0, j))]
    args = [scal, own, rem, ids_own, ids_rem]
    alias = {}
    if not first:
        in_specs += specs
        args += list(prev)
        alias = {5 + i: i for i in range(len(outs))}
    return pl.pallas_call(
        functools.partial(pair_kernel, want, first, sub),
        grid=(n_rem // blk,), in_specs=in_specs, out_specs=specs, out_shape=outs,
        input_output_aliases=alias,
        compiler_params=pltpu.CompilerParams(vmem_limit_bytes=56 << 20),
        cost_estimate=pl.CostEstimate(flops=4 * rows * n_rem * dim, bytes_accessed=2 * n_rem * dim, transcendentals=0),
    )(*args)


def solution(mesh):
    n_dev = mesh.shape["data"]
    chunks = 2

    def local_fn(feat_img, feat_txt, w_img, w_txt, log_temp, logit_bias, pair_ids):
        rows = feat_img.shape[0]
        dim = w_img.shape[1]
        total_rows = rows * n_dev
        temp_scale = jnp.exp(log_temp)
        scal = jnp.stack([-temp_scale * LOG2E, -logit_bias * LOG2E])
        unit_txt, inv_txt, emb_txt = embed_rows(feat_txt, w_txt)
        unit_img, inv_img, emb_img = embed_rows(feat_img, w_img)
        part = rows // chunks
        ids_all = lax.all_gather(pair_ids, "data")
        ids_own = pair_ids[:, None]

        def run_pass(own, other, want, sub):
            state = None
            for c in range(chunks):
                gathered = lax.all_gather(other[c * part:(c + 1) * part], "data", tiled=True)
                ids_rem = ids_all[:, c * part:(c + 1) * part].reshape(1, -1)
                state = pair_call(own, gathered, ids_own, ids_rem, scal, state, want, 1024, sub)
            return state

        acc_img, loss_sum, temp_sum, bias_sum = run_pass(emb_img, emb_txt, True, 256)
        (acc_txt,) = run_pass(emb_txt, emb_img, False, 512)
        factor = temp_scale / total_rows
        dw_img = weight_grad(feat_img, unit_img, inv_img, factor * acc_img)
        dw_txt = weight_grad(feat_txt, unit_txt, inv_txt, factor * acc_txt)
        sums = jnp.stack([jnp.sum(loss_sum), jnp.sum(temp_sum), jnp.sum(bias_sum)])
        sums, dw_img, dw_txt = lax.psum((sums, dw_img, dw_txt), "data")
        return (sums[0] / (LOG2E * total_rows), temp_scale * sums[1] / total_rows, sums[2] / total_rows, dw_img, dw_txt)

    return jax.shard_map(
        local_fn,
        mesh=mesh,
        in_specs=(P("data", None), P("data", None), P(None, None), P(None, None), P(), P(), P("data")),
        out_specs=(P(), P(), P(), P(None, None), P(None, None)),
        check_vma=False,
    )
```

```python
import functools

import jax
import jax.numpy as jnp
from jax import lax
from jax.experimental import pallas as pl
from jax.experimental.pallas import tpu as pltpu
from jax.sharding import PartitionSpec as P

CONTRACT_ROWS = (((0,), (0,)), ((), ()))
CONTRACT_COLS = (((1,), (1,)), ((), ()))
LOG2E = 1.4426950408889634
MESH_ID = pl.DeviceIdType.MESH

ROWS, DIM = 1024, 1152
TILE = 512
COLOR = DIM // 3
LINK_BITS = (2, 4, 8)
SLOTS = 16
ROW_PIECE = 32
D1_PIECE = (512, 256)
D2_PIECE = (512, 512)


def embed_rows(feat_rows, weights):
    raw_emb = jnp.dot(feat_rows, weights, preferred_element_type=jnp.float32)
    inv_norm = lax.rsqrt(jnp.sum(raw_emb * raw_emb, axis=1, keepdims=True))
    unit_emb = raw_emb * inv_norm
    return unit_emb, inv_norm, unit_emb.astype(jnp.bfloat16)


def weight_grad(feat_rows, unit_emb, inv_norm, grad_emb):
    raw_grad = inv_norm * (grad_emb - unit_emb * jnp.sum(unit_emb * grad_emb, axis=1, keepdims=True))
    return lax.dot_general(feat_rows, raw_grad.astype(jnp.bfloat16), CONTRACT_ROWS, preferred_element_type=jnp.float32)


def transfer_table(color):
    b0, b1, b2 = (LINK_BITS[(color + j) % 3] for j in range(3))
    return ((b0, 0), (b1, 0), (b1, b0), (b2, 0), (b2, b0), (b2, b1), (b2, b0 | b1))


def tile_order():
    order = [(0, 0), (1, 0), (0, 1), (1, 1)]
    groups = [((2, 4, 8), 0), ((2, 4, 8), 1), ((6, 10, 12), 0), ((6, 10, 12), 1), ((14,), 0), ((14,), 1)]
    for slots, half in groups:
        for slot in slots:
            order += [(slot, half), (slot | 1, half)]
    return order


ORDER = tile_order()
N_TILES = len(ORDER)


def interleave(first, second):
    i = j = 0
    while i < len(first) or j < len(second):
        if j >= len(second) or (i < len(first) and i * len(second) <= j * len(first)):
            first[i]()
            i += 1
        else:
            second[j]()
            j += 1


def d1_pieces(own, tile, sim_out):
    def piece(m, n):
        sim_out[m:m + D1_PIECE[0], n:n + D1_PIECE[1]] = lax.dot_general(
            own[m:m + D1_PIECE[0], :], tile[n:n + D1_PIECE[1], :], CONTRACT_COLS, preferred_element_type=jnp.float32)

    return [functools.partial(piece, m, n) for n in range(0, TILE, D1_PIECE[1]) for m in range(0, ROWS, D1_PIECE[0])]


def d2_pieces(grad, tile, acc):
    def piece(m, n, end):
        acc[m:m + D2_PIECE[0], n:end] += jnp.dot(
            grad[m:m + D2_PIECE[0], :], tile[:, n:end], preferred_element_type=jnp.float32)

    return [functools.partial(piece, m, n, min(n + D2_PIECE[1], DIM))
            for m in range(0, ROWS, D2_PIECE[0]) for n in range(0, DIM, D2_PIECE[1])]


def fold_cols(x):
    y = x[:, 0:128]
    for c in range(1, TILE // 128):
        y = y + x[:, c * 128:(c + 1) * 128]
    return y


def vpu_pieces(want, neg_scale, neg_bias, sim, grad_out, ids_own, ids_rem, sums):
    state = {}

    def add(name, value):
        state[name] = state[name] + value if name in state else value

    def piece(r0):
        s = sim[r0:r0 + ROW_PIECE, :]
        neg_y = jnp.where(ids_own[r0:r0 + ROW_PIECE, :] == ids_rem[...], -1.0, 1.0)
        yz = (s * neg_scale + neg_bias) * neg_y
        if want:
            e = jnp.exp2(-jnp.abs(yz))
            r = 1.0 / (1.0 + e)
            grad = jnp.where(yz <= 0, r, e * r) * neg_y
            low = jnp.minimum(yz, 0.0)
            gs = grad * s
            for i in range(0, ROW_PIECE, 8):
                e_i = e[i:i + 8]
                state["prod"] = state["prod"] + (e_i + state["prod"] * e_i) if "prod" in state else e_i
                add("low", low[i:i + 8])
                add("gs", gs[i:i + 8])
                add("g", grad[i:i + 8])
            if (r0 + ROW_PIECE) % 512 == 0:
                state["low"] = state["low"] - jnp.log1p(state.pop("prod")) * LOG2E
            if r0 + ROW_PIECE == ROWS:
                sums[0][...] -= fold_cols(state["low"])
                sums[1][...] += fold_cols(state["gs"])
                sums[2][...] += fold_cols(state["g"])
        else:
            grad = neg_y / (1.0 + jnp.exp2(yz))
        grad_out[r0:r0 + ROW_PIECE, :] = grad.astype(jnp.bfloat16)

    return [functools.partial(piece, r0) for r0 in range(0, ROWS, ROW_PIECE)]


def main_kernel(scal, emb_txt_hbm, emb_img_hbm, emb_txt, emb_img, ids_own, ids_row,
                acc_img, acc_txt, sum_l, sum_t, sum_b, gat,
                tiles, sim0, sim1, grad0, grad1, ids_all, ids_cur,
                send_sem, recv_sem, pair_send, pair_recv, ids_send, ids_recv, tile_sem):
    me = lax.axis_index("data")
    emb_hbm = (emb_txt_hbm, emb_img_hbm)
    sims, grads = (sim0, sim1), (grad0, grad1)
    sums = (sum_l, sum_t, sum_b)

    def flip(bit):
        return me + bit * (1 - 2 * lax.rem(lax.div(me, bit), 2))

    peer = {bit: flip(bit) for bit in (1, 2, 4, 8)}

    def xor_dev(slot):
        dev = me
        for bit in (1, 2, 4, 8):
            if slot & bit:
                dev = dev + (peer[bit] - me)
        return dev

    def rows_of(half):
        return pl.ds(half * TILE, TILE)

    def transfer(arr, half, color, i):
        link, slot = transfer_table(color)[i]
        cols = pl.ds(color * COLOR, COLOR)
        src = emb_hbm[arr].at[rows_of(half), cols] if slot == 0 else gat.at[arr, slot, rows_of(half), cols]
        return pltpu.make_async_remote_copy(
            src_ref=src, dst_ref=gat.at[arr, slot | link, rows_of(half), cols],
            send_sem=send_sem.at[arr, half, color, i], recv_sem=recv_sem.at[arr, half, color, i],
            device_id=(peer[link],), device_id_type=MESH_ID)

    def pair_copy(arr, half, slot):
        src = emb_hbm[arr].at[rows_of(half)] if slot == 0 else gat.at[arr, slot, rows_of(half)]
        return pltpu.make_async_remote_copy(
            src_ref=src, dst_ref=gat.at[arr, slot | 1, rows_of(half)],
            send_sem=pair_send.at[arr, half, slot // 2], recv_sem=pair_recv.at[arr, half, slot // 2],
            device_id=(peer[1],), device_id_type=MESH_ID)

    def ids_copy(slot):
        return pltpu.make_async_remote_copy(
            src_ref=ids_row, dst_ref=ids_all.at[slot], send_sem=ids_send.at[slot], recv_sem=ids_recv.at[slot],
            device_id=(xor_dev(slot),), device_id_type=MESH_ID)

    def send_own(arr, half):
        for j in range(3):
            for d in range(3):
                color = (d - j) % 3
                transfer(arr, half, color, (0, 1, 3)[j]).start()

    def arrived(arr, slot, half):
        if slot == 0:
            return
        if slot & 1:
            pair_copy(arr, half, slot - 1).wait_recv()
            return
        for color in range(3):
            table = transfer_table(color)
            for i, (link, src) in enumerate(table):
                if src | link == slot:
                    transfer(arr, half, color, i).wait_recv()
        for color in range(3):
            table = transfer_table(color)
            for i, (link, src) in enumerate(table):
                if src == slot:
                    transfer(arr, half, color, i).start()
        pair_copy(arr, half, slot).start()

    def tile_copy(u):
        arr, (slot, half) = u // N_TILES, ORDER[u % N_TILES]
        src = emb_hbm[arr].at[rows_of(half)] if slot == 0 else gat.at[arr, slot, rows_of(half)]
        return pltpu.make_async_copy(src, tiles.at[u % 4], tile_sem.at[u % 4])

    def comm(u):
        if u + 1 < 2 * N_TILES:
            arr, (slot, half) = (u + 1) // N_TILES, ORDER[(u + 1) % N_TILES]
            arrived(arr, slot, half)
            tile_copy(u + 1).start()
            if (arr, slot, half) == (0, 12, 1):
                for h in range(2):
                    send_own(1, h)
                    pair_copy(1, h, 0).start()
        if u < 2 * N_TILES:
            tile_copy(u).wait()
        if u >= 1:
            v = u - 1
            slot, half = ORDER[v % N_TILES]
            if v < N_TILES and half == 0 and slot:
                ids_copy(slot).wait_recv()
            src = ids_row if slot == 0 else ids_all.at[slot]
            ids_cur[...] = src[:, half * TILE:(half + 1) * TILE]

    neg_scale, neg_bias = scal[0], scal[1]

    def step(par, d1_arr, vpu_arr, d2_arr, cur_buf, old_buf):
        mxu, vpu = [], []
        if d1_arr is not None:
            mxu += d1_pieces((emb_img, emb_txt)[d1_arr], tiles.at[cur_buf], sims[par])
        if d2_arr is not None:
            mxu += d2_pieces(grads[par], tiles.at[old_buf], (acc_img, acc_txt)[d2_arr])
        if vpu_arr is not None:
            vpu = vpu_pieces(vpu_arr == 0, neg_scale, neg_bias, sims[1 - par], grads[1 - par], ids_own, ids_cur, sums)
        interleave(mxu, vpu)

    barrier = pltpu.get_barrier_semaphore()
    for slot in range(1, SLOTS):
        pl.semaphore_signal(barrier, inc=1, device_id=(xor_dev(slot),), device_id_type=MESH_ID)
    pl.semaphore_wait(barrier, SLOTS - 1)

    tile_copy(0).start()
    for slot in range(1, SLOTS):
        ids_copy(slot).start()
    for h in range(2):
        pair_copy(0, h, 0).start()
        send_own(0, h)

    acc_img[...] = jnp.zeros_like(acc_img)
    acc_txt[...] = jnp.zeros_like(acc_txt)
    for out in sums:
        out[...] = jnp.zeros_like(out)

    comm(0)
    step(0, 0, None, None, 0, 0)
    comm(1)
    step(1, 0, 0, None, 1, 0)

    def run_loop(arr, start):
        n_iter = (N_TILES - 2) // 2

        @pl.loop(0, n_iter)
        def _(it):
            flip_buf = lax.rem(it, 2)
            base = (start // 2) % 2
            buf = 2 * lax.rem(it + base, 2)
            for par in range(2):
                for k in range(n_iter):
                    pl.when(it == k)(functools.partial(comm, start + 2 * k + par))
                step(par, arr, arr, arr, buf + par, (2 - buf) + par)

    run_loop(0, 2)
    comm(N_TILES)
    step(0, 1, 0, 0, N_TILES % 4, (N_TILES - 2) % 4)
    comm(N_TILES + 1)
    step(1, 1, 1, 0, (N_TILES + 1) % 4, (N_TILES - 1) % 4)
    run_loop(1, N_TILES + 2)
    comm(2 * N_TILES)
    step(0, None, 1, 1, 0, (2 * N_TILES - 2) % 4)
    step(1, None, None, 1, 0, (2 * N_TILES - 1) % 4)

    for slot in range(1, SLOTS):
        ids_copy(slot).wait_send()
    for arr in range(2):
        for half in range(2):
            for color in range(3):
                for i in range(7):
                    transfer(arr, half, color, i).wait_send()
            for slot in range(0, SLOTS, 2):
                pair_copy(arr, half, slot).wait_send()


def main_call(scal, emb_txt, emb_img, ids):
    vmem = pl.BlockSpec(memory_space=pltpu.VMEM)
    hbm = pl.BlockSpec(memory_space=pl.ANY)
    f32 = jnp.float32
    return pl.pallas_call(
        main_kernel,
        in_specs=[pl.BlockSpec(memory_space=pltpu.SMEM), hbm, hbm, vmem, vmem, vmem, vmem],
        out_specs=[vmem] * 5 + [hbm],
        out_shape=[jax.ShapeDtypeStruct((ROWS, DIM), f32)] * 2 + [jax.ShapeDtypeStruct((8, 128), f32)] * 3
        + [jax.ShapeDtypeStruct((2, SLOTS, ROWS, DIM), jnp.bfloat16)],
        scratch_shapes=[
            pltpu.VMEM((4, TILE, DIM), jnp.bfloat16),
            pltpu.VMEM((ROWS, TILE), f32), pltpu.VMEM((ROWS, TILE), f32),
            pltpu.VMEM((ROWS, TILE), jnp.bfloat16), pltpu.VMEM((ROWS, TILE), jnp.bfloat16),
            pltpu.VMEM((SLOTS, 1, ROWS), jnp.int32), pltpu.VMEM((1, TILE), jnp.int32),
            pltpu.SemaphoreType.DMA((2, 2, 3, 7)), pltpu.SemaphoreType.DMA((2, 2, 3, 7)),
            pltpu.SemaphoreType.DMA((2, 2, 8)), pltpu.SemaphoreType.DMA((2, 2, 8)),
            pltpu.SemaphoreType.DMA((SLOTS,)), pltpu.SemaphoreType.DMA((SLOTS,)),
            pltpu.SemaphoreType.DMA((4,)),
        ],
        compiler_params=pltpu.CompilerParams(collective_id=0, has_side_effects=True, vmem_limit_bytes=60 << 20),
    )(scal, emb_txt, emb_img, emb_txt, emb_img, ids[:, None], ids[None, :])


def solution(mesh):
    n_dev = mesh.shape["data"]

    def local_fn(feat_img, feat_txt, w_img, w_txt, log_temp, logit_bias, pair_ids):
        total_rows = feat_img.shape[0] * n_dev
        temp_scale = jnp.exp(log_temp)
        scal = jnp.stack([-temp_scale * LOG2E, -logit_bias * LOG2E])
        unit_txt, inv_txt, emb_txt = embed_rows(feat_txt, w_txt)
        unit_img, inv_img, emb_img = embed_rows(feat_img, w_img)
        acc_img, acc_txt, loss_sum, temp_sum, bias_sum, _ = main_call(scal, emb_txt, emb_img, pair_ids)
        factor = temp_scale / total_rows
        dw_img = weight_grad(feat_img, unit_img, inv_img, factor * acc_img)
        dw_txt = weight_grad(feat_txt, unit_txt, inv_txt, factor * acc_txt)
        sums = jnp.stack([jnp.sum(loss_sum), jnp.sum(temp_sum), jnp.sum(bias_sum)])
        sums, dw_img, dw_txt = lax.psum((sums, dw_img, dw_txt), "data")
        return (sums[0] / (LOG2E * total_rows), temp_scale * sums[1] / total_rows, sums[2] / total_rows, dw_img, dw_txt)

    return jax.shard_map(
        local_fn,
        mesh=mesh,
        in_specs=(P("data", None), P("data", None), P(None, None), P(None, None), P(), P(), P("data")),
        out_specs=(P(), P(), P(), P(None, None), P(None, None)),
        check_vma=False,
    )
```

```python
import functools

import jax
import jax.numpy as jnp
from jax import lax
from jax.experimental import pallas as pl
from jax.experimental.pallas import tpu as pltpu
from jax.sharding import PartitionSpec as P

CONTRACT_ROWS = (((0,), (0,)), ((), ()))
CONTRACT_COLS = (((1,), (1,)), ((), ()))
LOG2E = 1.4426950408889634
MESH_ID = pl.DeviceIdType.MESH

ROWS, DIM = 1024, 1152
TILE = 512
COLOR = DIM // 3
LINK_BITS = (2, 4, 8)
SLOTS = 16
ROW_PIECE = 32
D1_PIECE = (512, 256)
D2_PIECE = (512, 512)
HALF_DIM = DIM // 2
RS_ROWS = (HALF_DIM // 2, HALF_DIM // 4, HALF_DIM // 8)
REDUCE_STEPS = {50: 1, 53: 2, 55: 3, 57: 4, 59: 5, 61: 6, 64: 7}


def transfer_table(color):
    b0, b1, b2 = (LINK_BITS[(color + j) % 3] for j in range(3))
    return ((b0, 0), (b1, 0), (b1, b0), (b2, 0), (b2, b0), (b2, b1), (b2, b0 | b1))


def tile_order():
    order = [(0, 0), (1, 0), (0, 1), (1, 1)]
    groups = [((2, 4, 8), 0), ((2, 4, 8), 1), ((6, 10, 12), 0), ((6, 10, 12), 1), ((14,), 0), ((14,), 1)]
    for slots, half in groups:
        for slot in slots:
            order += [(slot, half), (slot | 1, half)]
    return order


ORDER = tile_order()
N_TILES = len(ORDER)


def interleave(first, second):
    i = j = 0
    while i < len(first) or j < len(second):
        if j >= len(second) or (i < len(first) and i * len(second) <= j * len(first)):
            first[i]()
            i += 1
        else:
            second[j]()
            j += 1


def d1_pieces(own, tile, sim_out):
    def piece(m, n):
        sim_out[m:m + D1_PIECE[0], n:n + D1_PIECE[1]] = lax.dot_general(
            own[m:m + D1_PIECE[0], :], tile[n:n + D1_PIECE[1], :], CONTRACT_COLS, preferred_element_type=jnp.float32)

    return [functools.partial(piece, m, n) for n in range(0, TILE, D1_PIECE[1]) for m in range(0, ROWS, D1_PIECE[0])]


def d2_pieces(grad, tile, acc):
    def piece(m, n, end):
        acc[m:m + D2_PIECE[0], n:end] += jnp.dot(
            grad[m:m + D2_PIECE[0], :], tile[:, n:end], preferred_element_type=jnp.float32)

    return [functools.partial(piece, m, n, min(n + D2_PIECE[1], DIM))
            for m in range(0, ROWS, D2_PIECE[0]) for n in range(0, DIM, D2_PIECE[1])]


def fold_cols(x):
    y = x[:, 0:128]
    for c in range(1, TILE // 128):
        y = y + x[:, c * 128:(c + 1) * 128]
    return y


def vpu_pieces(want, neg_scale, neg_bias, sim, grad_out, ids_own, ids_rem, sums):
    state = {}

    def add(name, value):
        state[name] = state[name] + value if name in state else value

    def piece(r0):
        s = sim[r0:r0 + ROW_PIECE, :]
        neg_y = jnp.where(ids_own[r0:r0 + ROW_PIECE, :] == ids_rem[...], -1.0, 1.0)
        yz = (s * neg_scale + neg_bias) * neg_y
        if want:
            e = jnp.exp2(-jnp.abs(yz))
            r = 1.0 / (1.0 + e)
            grad = jnp.where(yz <= 0, r, e * r) * neg_y
            low = jnp.minimum(yz, 0.0)
            gs = grad * s
            for i in range(0, ROW_PIECE, 8):
                e_i = e[i:i + 8]
                state["prod"] = state["prod"] + (e_i + state["prod"] * e_i) if "prod" in state else e_i
                add("low", low[i:i + 8])
                add("gs", gs[i:i + 8])
                add("g", grad[i:i + 8])
            if (r0 + ROW_PIECE) % 512 == 0:
                state["low"] = state["low"] - jnp.log1p(state.pop("prod")) * LOG2E
            if r0 + ROW_PIECE == ROWS:
                sums[0][...] -= fold_cols(state["low"])
                sums[1][...] += fold_cols(state["gs"])
                sums[2][...] += fold_cols(state["g"])
        else:
            grad = neg_y / (1.0 + jnp.exp2(yz))
        grad_out[r0:r0 + ROW_PIECE, :] = grad.astype(jnp.bfloat16)

    return [functools.partial(piece, r0) for r0 in range(0, ROWS, ROW_PIECE)]


def main_kernel(scal, feat_txt, feat_img, w_txt, w_img, ids_own, ids_row,
                dw_img, dw_txt, totals, gat, unit_hbm,
                feat0, feat1, wgt, part, unit, inv0, inv1, emb_txt, emb_img, acc_img, acc_txt,
                tiles, sim0, sim1, grad0, grad1, ids_all, ids_cur, sums_all, rx_pair, rx1, rx2, rx3,
                send_sem, recv_sem, pair_send, pair_recv, ids_send, ids_recv, tile_sem, load_sem, unit_sem, own_sem,
                sum_send, sum_recv, half_send, half_recv, ring_send, ring_recv):
    me = lax.axis_index("data")
    embs = (emb_txt, emb_img)
    feats, invs = (feat0, feat1), (inv0, inv1)
    sims, grads = (sim0, sim1), (grad0, grad1)
    sums = tuple(sums_all.at[0, i] for i in range(3))
    neg_scale, neg_bias, factor = scal[0], scal[1], scal[2]

    def bit_of(bit):
        return lax.rem(lax.div(me, bit), 2)

    peer = {bit: me + bit * (1 - 2 * bit_of(bit)) for bit in (1, 2, 4, 8)}

    def xor_dev(slot):
        dev = me
        for bit in (1, 2, 4, 8):
            if slot & bit:
                dev = dev + (peer[bit] - me)
        return dev

    def remote(src, dst, send, recv, dev):
        return pltpu.make_async_remote_copy(src_ref=src, dst_ref=dst, send_sem=send, recv_sem=recv,
                                            device_id=(dev,), device_id_type=MESH_ID)

    def rows_of(half):
        return pl.ds(half * TILE, TILE)

    def transfer(arr, half, color, i):
        link, slot = transfer_table(color)[i]
        cols = pl.ds(color * COLOR, COLOR)
        return remote(gat.at[arr, slot, rows_of(half), cols], gat.at[arr, slot | link, rows_of(half), cols],
                      send_sem.at[arr, half, color, i], recv_sem.at[arr, half, color, i], peer[link])

    def pair_copy(arr, half, slot):
        return remote(gat.at[arr, slot, rows_of(half)], gat.at[arr, slot | 1, rows_of(half)],
                      pair_send.at[arr, half, slot // 2], pair_recv.at[arr, half, slot // 2], peer[1])

    def ids_copy(slot):
        return remote(ids_row, ids_all.at[slot], ids_send.at[slot], ids_recv.at[slot], xor_dev(slot))

    def sums_copy(slot):
        return remote(sums_all.at[0], sums_all.at[slot], sum_send.at[slot], sum_recv.at[slot], xor_dev(slot))

    def send_own(arr, half):
        pair_copy(arr, half, 0).start()
        for j in range(3):
            for d in range(3):
                color = (d - j) % 3
                transfer(arr, half, color, (0, 1, 3)[j]).start()

    def arrived(arr, slot, half):
        if slot == 0:
            return
        if slot & 1:
            pair_copy(arr, half, slot - 1).wait_recv()
            return
        for color in range(3):
            for i, (link, src) in enumerate(transfer_table(color)):
                if src | link == slot:
                    transfer(arr, half, color, i).wait_recv()
        for color in range(3):
            for i, (link, src) in enumerate(transfer_table(color)):
                if src == slot:
                    transfer(arr, half, color, i).start()
        pair_copy(arr, half, slot).start()

    dws = (dw_img, dw_txt)
    rxs = (rx1, rx2, rx3)

    def half_copy(arr, last):
        core = bit_of(1)
        start = HALF_DIM * (core if last else 1 - core)
        src = (dws[arr] if last else part).at[pl.ds(pl.multiple_of(start, 8), HALF_DIM)]
        return remote(src, src if last else rx_pair, half_send.at[arr, last], half_recv.at[arr, last], peer[1])

    def ring_offset(color, depth, flip_last):
        off = HALF_DIM * bit_of(1)
        for j in range(depth):
            bit = bit_of(LINK_BITS[(color + j) % 3])
            if flip_last and j == depth - 1:
                bit = 1 - bit
            off = off + RS_ROWS[j] * bit
        return pl.multiple_of(off, 8)

    def ring_copy(arr, color, phase):
        cols = pl.ds(color * COLOR, COLOR)
        if phase < 3:
            rows = pl.ds(ring_offset(color, phase + 1, True), RS_ROWS[phase])
            src, dst, dim = part.at[rows, cols], rxs[phase].at[color], phase
        else:
            dim = 5 - phase
            rows = pl.ds(ring_offset(color, dim + 1, False), RS_ROWS[dim])
            src = dst = dws[arr].at[rows, cols]
        return remote(src, dst, ring_send.at[arr, color, phase], ring_recv.at[arr, color, phase],
                      peer[LINK_BITS[(color + dim) % 3]])

    def reduce_phase(arr, phase):
        if phase == 0:
            half_copy(arr, 0).start()
            return
        if phase == 1:
            half_copy(arr, 0).wait_recv()
            base = HALF_DIM * bit_of(1)

            @pl.loop(0, HALF_DIM // 32)
            def _(i):
                rows = pl.ds(pl.multiple_of(base + i * 32, 8), 32)
                part[rows, :] += rx_pair[pl.ds(pl.multiple_of(i * 32, 8), 32), :]

            for color in range(3):
                ring_copy(arr, color, 0).start()
            return
        if phase <= 4:
            done = phase - 2
            n_rows = RS_ROWS[done]
            for color in range(3):
                ring_copy(arr, color, done).wait_recv()
                cols = pl.ds(color * COLOR, COLOR)
                base = ring_offset(color, done + 1, False)

                @pl.loop(0, n_rows // 24)
                def _(i):
                    rows = pl.ds(pl.multiple_of(base + i * 24, 8), 24)
                    total = part[rows, cols] + rxs[done][color, pl.ds(pl.multiple_of(i * 24, 8), 24), :]
                    (dws[arr] if done == 2 else part)[rows, cols] = total

                ring_copy(arr, color, done + 1).start()
            return
        if phase <= 6:
            for color in range(3):
                ring_copy(arr, color, phase - 2).wait_recv()
                ring_copy(arr, color, phase - 1).start()
            return
        if phase == 7:
            for color in range(3):
                ring_copy(arr, color, 5).wait_recv()
            half_copy(arr, 1).start()
            return
        half_copy(arr, 1).wait_recv()
        for last in range(2):
            half_copy(arr, last).wait_send()
        for color in range(3):
            for ph in range(6):
                ring_copy(arr, color, ph).wait_send()

    def load(arr, which):
        src, dst = (((feat_txt, feat0), (w_txt, wgt)), ((feat_img, feat1), (w_img, wgt)))[arr][which]
        return pltpu.make_async_copy(src, dst, load_sem.at[arr, which])

    def own_copy(arr, half):
        return pltpu.make_async_copy(embs[arr].at[rows_of(half)], gat.at[arr, 0, rows_of(half)], own_sem.at[arr, half])

    def embed_half(arr, half):
        rows = rows_of(half)
        raw = jnp.dot(feats[arr][rows, :], wgt[...], preferred_element_type=jnp.float32)
        inv = lax.rsqrt(jnp.sum(raw * raw, axis=1, keepdims=True))
        unit_rows = raw * inv
        unit[rows, :] = unit_rows
        invs[arr][rows, :] = inv
        embs[arr][rows, :] = unit_rows.astype(jnp.bfloat16)
        own_copy(arr, half).start()

    def finish(arr, acc):
        @pl.loop(0, ROWS // 64)
        def _(i):
            rows = pl.ds(pl.multiple_of(i * 64, 64), 64)
            grad = factor * acc[rows, :]
            unit_rows = unit[rows, :]
            proj = jnp.sum(unit_rows * grad, axis=1, keepdims=True)
            embs[arr][rows, :] = (invs[arr][rows, :] * (grad - unit_rows * proj)).astype(jnp.bfloat16)

        part[...] = lax.dot_general(feats[arr][...], embs[arr][...], CONTRACT_ROWS, preferred_element_type=jnp.float32)

    def tile_copy(u):
        arr, (slot, half) = u // N_TILES, ORDER[u % N_TILES]
        return pltpu.make_async_copy(gat.at[arr, slot, rows_of(half)], tiles.at[u % 4], tile_sem.at[u % 4])

    def comm(u):
        if u + 1 < 2 * N_TILES:
            arr, (slot, half) = (u + 1) // N_TILES, ORDER[(u + 1) % N_TILES]
            arrived(arr, slot, half)
            tile_copy(u + 1).start()
            if (arr, slot, half) == (0, 12, 1):
                for h in range(2):
                    send_own(1, h)
        if u in REDUCE_STEPS:
            reduce_phase(0, REDUCE_STEPS[u])
        if u < 2 * N_TILES:
            tile_copy(u).wait()
        if u >= 1:
            v = u - 1
            slot, half = ORDER[v % N_TILES]
            if v < N_TILES and half == 0 and slot:
                ids_copy(slot).wait_recv()
            src = ids_row if slot == 0 else ids_all.at[slot]
            ids_cur[...] = src[:, half * TILE:(half + 1) * TILE]

    def step(par, d1_arr, vpu_arr, d2_arr, cur_buf, old_buf):
        mxu, vpu = [], []
        if d1_arr is not None:
            mxu += d1_pieces((emb_img, emb_txt)[d1_arr], tiles.at[cur_buf], sims[par])
        if d2_arr is not None:
            mxu += d2_pieces(grads[par], tiles.at[old_buf], (acc_img, acc_txt)[d2_arr])
        if vpu_arr is not None:
            vpu = vpu_pieces(vpu_arr == 0, neg_scale, neg_bias, sims[1 - par], grads[1 - par],
                             ids_own, ids_cur, sums)
        interleave(mxu, vpu)

    load(0, 0).start()
    load(0, 1).start()
    load(1, 0).start()
    barrier = pltpu.get_barrier_semaphore()
    for slot in range(1, SLOTS):
        pl.semaphore_signal(barrier, inc=1, device_id=(xor_dev(slot),), device_id_type=MESH_ID)
    load(0, 0).wait()
    load(0, 1).wait()
    embed_half(0, 0)
    pl.semaphore_wait(barrier, SLOTS - 1)
    own_copy(0, 0).wait()
    send_own(0, 0)
    tile_copy(0).start()
    for slot in range(1, SLOTS):
        ids_copy(slot).start()
    embed_half(0, 1)
    load(1, 1).start()
    own_copy(0, 1).wait()
    send_own(0, 1)
    unit_out = pltpu.make_async_copy(unit, unit_hbm, unit_sem.at[0])
    unit_out.start()
    acc_img[...] = jnp.zeros_like(acc_img)
    acc_txt[...] = jnp.zeros_like(acc_txt)
    for out in sums:
        out[...] = jnp.zeros(out.shape, jnp.float32)
    load(1, 0).wait()
    load(1, 1).wait()
    unit_out.wait()
    for half in range(2):
        embed_half(1, half)
    for half in range(2):
        own_copy(1, half).wait()

    comm(0)
    step(0, 0, None, None, 0, 0)
    comm(1)
    step(1, 0, 0, None, 1, 0)

    def run_loop(arr, start):
        n_iter = (N_TILES - 2) // 2

        @pl.loop(0, n_iter)
        def _(it):
            base = (start // 2) % 2
            buf = 2 * lax.rem(it + base, 2)
            for par in range(2):
                for k in range(n_iter):
                    pl.when(it == k)(functools.partial(comm, start + 2 * k + par))
                step(par, arr, arr, arr, buf + par, (2 - buf) + par)

    run_loop(0, 2)
    comm(N_TILES)
    step(0, 1, 0, 0, N_TILES % 4, (N_TILES - 2) % 4)
    for slot in range(1, SLOTS):
        sums_copy(slot).start()
    comm(N_TILES + 1)
    step(1, 1, 1, 0, (N_TILES + 1) % 4, (N_TILES - 1) % 4)
    finish(1, acc_img)
    reduce_phase(0, 0)
    unit_in = pltpu.make_async_copy(unit_hbm, unit, unit_sem.at[1])
    unit_in.start()
    run_loop(1, N_TILES + 2)
    comm(2 * N_TILES)
    step(0, None, 1, 1, 0, (2 * N_TILES - 2) % 4)
    step(1, None, None, 1, 0, (2 * N_TILES - 1) % 4)
    reduce_phase(0, 8)
    unit_in.wait()
    finish(0, acc_txt)
    reduce_phase(1, 0)

    for slot in range(1, SLOTS):
        sums_copy(slot).wait_recv()
    for i in range(3):
        parts = [sums_all[slot, i] for slot in range(SLOTS)]
        while len(parts) > 1:
            parts = [parts[j] + parts[j + 1] for j in range(0, len(parts), 2)]
        totals[i] = parts[0]
    for phase in range(1, 9):
        reduce_phase(1, phase)

    for slot in range(1, SLOTS):
        ids_copy(slot).wait_send()
        sums_copy(slot).wait_send()
    for arr in range(2):
        for half in range(2):
            for color in range(3):
                for i in range(7):
                    transfer(arr, half, color, i).wait_send()
            for slot in range(0, SLOTS, 2):
                pair_copy(arr, half, slot).wait_send()


def main_call(scal, feat_txt, feat_img, w_txt, w_img, ids):
    vmem = pl.BlockSpec(memory_space=pltpu.VMEM)
    hbm = pl.BlockSpec(memory_space=pl.ANY)
    f32, bf16 = jnp.float32, jnp.bfloat16
    dma = pltpu.SemaphoreType.DMA
    return pl.pallas_call(
        main_kernel,
        in_specs=[pl.BlockSpec(memory_space=pltpu.SMEM)] + [hbm] * 4 + [vmem] * 2,
        out_specs=[vmem] * 3 + [hbm] * 2,
        out_shape=[jax.ShapeDtypeStruct((DIM, DIM), f32)] * 2 + [jax.ShapeDtypeStruct((3, 8, 128), f32)]
        + [jax.ShapeDtypeStruct((2, SLOTS, ROWS, DIM), bf16), jax.ShapeDtypeStruct((ROWS, DIM), f32)],
        scratch_shapes=[
            pltpu.VMEM((ROWS, DIM), bf16), pltpu.VMEM((ROWS, DIM), bf16),
            pltpu.VMEM((DIM, DIM), bf16), pltpu.VMEM((DIM, DIM), f32),
            pltpu.VMEM((ROWS, DIM), f32), pltpu.VMEM((ROWS, 1), f32), pltpu.VMEM((ROWS, 1), f32),
            pltpu.VMEM((ROWS, DIM), bf16), pltpu.VMEM((ROWS, DIM), bf16),
            pltpu.VMEM((ROWS, DIM), f32), pltpu.VMEM((ROWS, DIM), f32),
            pltpu.VMEM((4, TILE, DIM), bf16),
            pltpu.VMEM((ROWS, TILE), f32), pltpu.VMEM((ROWS, TILE), f32),
            pltpu.VMEM((ROWS, TILE), bf16), pltpu.VMEM((ROWS, TILE), bf16),
            pltpu.VMEM((SLOTS, 1, ROWS), jnp.int32), pltpu.VMEM((1, TILE), jnp.int32),
            pltpu.VMEM((SLOTS, 3, 8, 128), f32), pltpu.VMEM((HALF_DIM, DIM), f32),
            pltpu.VMEM((3, RS_ROWS[0], COLOR), f32), pltpu.VMEM((3, RS_ROWS[1], COLOR), f32),
            pltpu.VMEM((3, RS_ROWS[2], COLOR), f32),
            dma((2, 2, 3, 7)), dma((2, 2, 3, 7)), dma((2, 2, 8)), dma((2, 2, 8)), dma((SLOTS,)), dma((SLOTS,)),
            dma((4,)), dma((2, 2)), dma((2,)), dma((2, 2)), dma((SLOTS,)), dma((SLOTS,)),
            dma((2, 2)), dma((2, 2)), dma((2, 3, 6)), dma((2, 3, 6)),
        ],
        compiler_params=pltpu.CompilerParams(collective_id=0, has_side_effects=True, vmem_limit_bytes=67043328),
    )(scal, feat_txt, feat_img, w_txt, w_img, ids[:, None], ids[None, :])


def solution(mesh):
    n_dev = mesh.shape["data"]

    def local_fn(feat_img, feat_txt, w_img, w_txt, log_temp, logit_bias, pair_ids):
        total_rows = feat_img.shape[0] * n_dev
        temp_scale = jnp.exp(log_temp)
        scal = jnp.stack([-temp_scale * LOG2E, -logit_bias * LOG2E, temp_scale / total_rows])
        dw_img, dw_txt, totals = main_call(scal, feat_txt, feat_img, w_txt, w_img, pair_ids)[:3]
        sums = jnp.sum(totals, axis=(1, 2))
        return (sums[0] / (LOG2E * total_rows), temp_scale * sums[1] / total_rows, sums[2] / total_rows, dw_img, dw_txt)

    return jax.shard_map(
        local_fn,
        mesh=mesh,
        in_specs=(P("data", None), P("data", None), P(None, None), P(None, None), P(), P(), P("data")),
        out_specs=(P(), P(), P(), P(None, None), P(None, None)),
        check_vma=False,
    )
```

```python
import functools

import jax
import jax.numpy as jnp
from jax import lax
from jax.experimental import pallas as pl
from jax.experimental.pallas import tpu as pltpu
from jax.sharding import PartitionSpec as P

CONTRACT_ROWS = (((0,), (0,)), ((), ()))
CONTRACT_COLS = (((1,), (1,)), ((), ()))
LOG2E = 1.4426950408889634
MESH_ID = pl.DeviceIdType.MESH

ROWS, DIM = 1024, 1152
TILE = 512
COLOR = DIM // 3
LINK_BITS = (2, 4, 8)
SLOTS = 16
ROW_PIECE = 128
D1_PIECE = (256, 512)
D2_PIECE = (512, 512)
HALF_DIM = DIM // 2
RS_ROWS = (HALF_DIM // 2, HALF_DIM // 4, HALF_DIM // 8)
REDUCE_STEPS = {54: 1, 57: 2, 59: 3, 60: 4, 61: 5, 62: 6, 64: 7}


def transfer_table(color):
    b0, b1, b2 = (LINK_BITS[(color + j) % 3] for j in range(3))
    return ((b0, 0), (b1, 0), (b1, b0), (b2, 0), (b2, b0), (b2, b1), (b2, b0 | b1))


def tile_order():
    order = [(0, 0), (1, 0), (0, 1), (1, 1)]
    groups = [((2, 4, 8), 0), ((2, 4, 8), 1), ((6, 10, 12), 0), ((6, 10, 12), 1), ((14,), 0), ((14,), 1)]
    for slots, half in groups:
        for slot in slots:
            order += [(slot, half), (slot | 1, half)]
    return order


ORDER = tile_order()
N_TILES = len(ORDER)


def interleave(first, second):
    i = j = 0
    while i < len(first) or j < len(second):
        if j >= len(second) or (i < len(first) and i * len(second) <= j * len(first)):
            first[i]()
            i += 1
        else:
            second[j]()
            j += 1


def d1_pieces(own, tile, sim_out):
    def piece(m, n):
        sim_out[m:m + D1_PIECE[0], n:n + D1_PIECE[1]] = lax.dot_general(
            own[m:m + D1_PIECE[0], :], tile[n:n + D1_PIECE[1], :], CONTRACT_COLS, preferred_element_type=jnp.float32)

    return [functools.partial(piece, m, n) for n in range(0, TILE, D1_PIECE[1]) for m in range(0, ROWS, D1_PIECE[0])]


def d2_pieces(grad, tile, acc):
    def piece(m, n, end):
        acc[m:m + D2_PIECE[0], n:end] += jnp.dot(
            grad[m:m + D2_PIECE[0], :], tile[:, n:end], preferred_element_type=jnp.float32)

    return [functools.partial(piece, m, n, min(n + D2_PIECE[1], DIM))
            for m in range(0, ROWS, D2_PIECE[0]) for n in range(0, DIM, D2_PIECE[1])]


def vpu_pieces(want, neg_scale, neg_bias, sim, grad_out, ids_own, ids_rem, sums):
    state = {"terms": 0}

    def add(name, value):
        state[name] = state[name] + value if name in state else value

    def chunk(r0, c0):
        rows, cols = slice(r0, r0 + ROW_PIECE), slice(c0, c0 + 128)
        s = sim[rows, cols]
        neg_y = jnp.where(ids_own[rows, :] == ids_rem[:, cols], -1.0, 1.0)
        yz = (s * neg_scale + neg_bias) * neg_y
        if want:
            e = jnp.exp2(-jnp.abs(yz))
            r = 1.0 / (1.0 + e)
            grad = jnp.where(yz <= 0, r, e * r) * neg_y
            low = jnp.minimum(yz, 0.0)
            gs = grad * s
            while e.shape[0] > 8:
                mid = e.shape[0] // 2
                e = e[:mid] + (e[mid:] + e[:mid] * e[mid:])
            state["prod"] = state["prod"] + (e + state["prod"] * e) if "prod" in state else e
            state["terms"] += ROW_PIECE // 8
            add("low", jnp.sum(low.reshape(-1, 8, 128), axis=0))
            add("gs", jnp.sum(gs.reshape(-1, 8, 128), axis=0))
            add("g", jnp.sum(grad.reshape(-1, 8, 128), axis=0))
            if state["terms"] == 64:
                state["low"] = state["low"] - jnp.log1p(state.pop("prod")) * LOG2E
                state["terms"] = 0
        else:
            grad = neg_y / (1.0 + jnp.exp2(yz))
        grad_out[rows, cols] = grad.astype(jnp.bfloat16)

    def piece(r0):
        for c0 in range(0, TILE, 128):
            chunk(r0, c0)
        if want and r0 + ROW_PIECE == ROWS:
            sums[0][...] -= state["low"]
            sums[1][...] += state["gs"]
            sums[2][...] += state["g"]

    return [functools.partial(piece, r0) for r0 in range(0, ROWS, ROW_PIECE)]


def ids_column(row):
    shape = (128, 128)
    diagonal = lax.broadcasted_iota(jnp.int32, shape, 0) == lax.broadcasted_iota(jnp.int32, shape, 1)
    picked = jnp.where(diagonal, jnp.broadcast_to(row.astype(jnp.float32), shape), 0.0)
    return jnp.broadcast_to(jnp.sum(picked, axis=1, keepdims=True), shape).astype(jnp.int32)


def main_kernel(scal, feat_txt, feat_img, w_txt, w_img, ids_row,
                dw_img, dw_txt, totals, gat, unit_hbm,
                ids_own, feat0, feat1, wgt, part, unit, inv0, inv1, emb_txt, emb_img, acc_img, acc_txt,
                tiles, sim0, sim1, grad0, grad1, ids_all, ids_cur, sums_all, rx_pair, rx1, rx2, rx3,
                send_sem, recv_sem, pair_send, pair_recv, ids_send, ids_recv, tile_sem, load_sem, unit_sem, own_sem,
                sum_send, sum_recv, half_send, half_recv, ring_send, ring_recv):
    me = lax.axis_index("data")
    embs = (emb_txt, emb_img)
    feats, invs = (feat0, feat1), (inv0, inv1)
    sims, grads = (sim0, sim1), (grad0, grad1)
    sums = tuple(sums_all.at[0, i] for i in range(3))
    neg_scale, neg_bias, factor = scal[0], scal[1], scal[2]

    def bit_of(bit):
        return lax.rem(lax.div(me, bit), 2)

    peer = {bit: me + bit * (1 - 2 * bit_of(bit)) for bit in (1, 2, 4, 8)}

    def xor_dev(slot):
        dev = me
        for bit in (1, 2, 4, 8):
            if slot & bit:
                dev = dev + (peer[bit] - me)
        return dev

    def remote(src, dst, send, recv, dev):
        return pltpu.make_async_remote_copy(src_ref=src, dst_ref=dst, send_sem=send, recv_sem=recv,
                                            device_id=(dev,), device_id_type=MESH_ID)

    def rows_of(half):
        return pl.ds(half * TILE, TILE)

    def transfer(arr, half, color, i):
        link, slot = transfer_table(color)[i]
        cols = pl.ds(color * COLOR, COLOR)
        return remote(gat.at[arr, slot, rows_of(half), cols], gat.at[arr, slot | link, rows_of(half), cols],
                      send_sem.at[arr, half, color, i], recv_sem.at[arr, half, color, i], peer[link])

    def pair_copy(arr, half, slot):
        return remote(gat.at[arr, slot, rows_of(half)], gat.at[arr, slot | 1, rows_of(half)],
                      pair_send.at[arr, half, slot // 2], pair_recv.at[arr, half, slot // 2], peer[1])

    def ids_copy(slot):
        return remote(ids_row, ids_all.at[slot], ids_send.at[slot], ids_recv.at[slot], xor_dev(slot))

    def sums_copy(slot):
        return remote(sums_all.at[0], sums_all.at[slot], sum_send.at[slot], sum_recv.at[slot], xor_dev(slot))

    def send_own(arr, half):
        pair_copy(arr, half, 0).start()
        for j in range(3):
            for d in range(3):
                color = (d - j) % 3
                transfer(arr, half, color, (0, 1, 3)[j]).start()

    def arrived(arr, slot, half):
        if slot == 0:
            return
        if slot & 1:
            pair_copy(arr, half, slot - 1).wait_recv()
            return
        for color in range(3):
            for i, (link, src) in enumerate(transfer_table(color)):
                if src | link == slot:
                    transfer(arr, half, color, i).wait_recv()
        for color in range(3):
            for i, (link, src) in enumerate(transfer_table(color)):
                if src == slot:
                    transfer(arr, half, color, i).start()
        pair_copy(arr, half, slot).start()

    dws = (dw_img, dw_txt)
    rxs = (rx1, rx2, rx3)

    def half_copy(arr, last):
        core = bit_of(1)
        start = HALF_DIM * (core if last else 1 - core)
        src = (dws[arr] if last else part).at[pl.ds(pl.multiple_of(start, 8), HALF_DIM)]
        return remote(src, src if last else rx_pair, half_send.at[arr, last], half_recv.at[arr, last], peer[1])

    def ring_offset(color, depth, flip_last):
        off = HALF_DIM * bit_of(1)
        for j in range(depth):
            bit = bit_of(LINK_BITS[(color + j) % 3])
            if flip_last and j == depth - 1:
                bit = 1 - bit
            off = off + RS_ROWS[j] * bit
        return pl.multiple_of(off, 8)

    def ring_copy(arr, color, phase):
        cols = pl.ds(color * COLOR, COLOR)
        if phase < 3:
            rows = pl.ds(ring_offset(color, phase + 1, True), RS_ROWS[phase])
            src, dst, dim = part.at[rows, cols], rxs[phase].at[color], phase
        else:
            dim = 5 - phase
            rows = pl.ds(ring_offset(color, dim + 1, False), RS_ROWS[dim])
            src = dst = dws[arr].at[rows, cols]
        return remote(src, dst, ring_send.at[arr, color, phase], ring_recv.at[arr, color, phase],
                      peer[LINK_BITS[(color + dim) % 3]])

    def reduce_phase(arr, phase):
        if phase == 0:
            half_copy(arr, 0).start()
            return
        if phase == 1:
            half_copy(arr, 0).wait_recv()
            base = HALF_DIM * bit_of(1)

            @pl.loop(0, HALF_DIM // 32)
            def _(i):
                rows = pl.ds(pl.multiple_of(base + i * 32, 8), 32)
                part[rows, :] += rx_pair[pl.ds(pl.multiple_of(i * 32, 8), 32), :]

            for color in range(3):
                ring_copy(arr, color, 0).start()
            return
        if phase <= 4:
            done = phase - 2
            n_rows = RS_ROWS[done]
            for color in range(3):
                ring_copy(arr, color, done).wait_recv()
                cols = pl.ds(color * COLOR, COLOR)
                base = ring_offset(color, done + 1, False)

                @pl.loop(0, n_rows // 24)
                def _(i):
                    rows = pl.ds(pl.multiple_of(base + i * 24, 8), 24)
                    total = part[rows, cols] + rxs[done][color, pl.ds(pl.multiple_of(i * 24, 8), 24), :]
                    (dws[arr] if done == 2 else part)[rows, cols] = total

                ring_copy(arr, color, done + 1).start()
            return
        if phase <= 6:
            for color in range(3):
                ring_copy(arr, color, phase - 2).wait_recv()
                ring_copy(arr, color, phase - 1).start()
            return
        if phase == 7:
            for color in range(3):
                ring_copy(arr, color, 5).wait_recv()
            half_copy(arr, 1).start()
            return
        half_copy(arr, 1).wait_recv()
        for last in range(2):
            half_copy(arr, last).wait_send()
        for color in range(3):
            for ph in range(6):
                ring_copy(arr, color, ph).wait_send()

    def load(arr, which):
        src, dst = (((feat_txt, feat0), (w_txt, wgt)), ((feat_img, feat1), (w_img, wgt)))[arr][which]
        return pltpu.make_async_copy(src, dst, load_sem.at[arr, which])

    def own_copy(arr, half):
        return pltpu.make_async_copy(embs[arr].at[rows_of(half)], gat.at[arr, 0, rows_of(half)], own_sem.at[arr, half])

    def embed_half(arr, half):
        rows = rows_of(half)
        raw = jnp.dot(feats[arr][rows, :], wgt[...], preferred_element_type=jnp.float32)
        inv = lax.rsqrt(jnp.sum(raw * raw, axis=1, keepdims=True))
        unit_rows = raw * inv
        unit[rows, :] = unit_rows
        invs[arr][rows, :] = inv
        embs[arr][rows, :] = unit_rows.astype(jnp.bfloat16)
        own_copy(arr, half).start()

    def finish(arr, acc):
        @pl.loop(0, ROWS // 64)
        def _(i):
            rows = pl.ds(pl.multiple_of(i * 64, 64), 64)
            grad = factor * acc[rows, :]
            unit_rows = unit[rows, :]
            proj = jnp.sum(unit_rows * grad, axis=1, keepdims=True)
            embs[arr][rows, :] = (invs[arr][rows, :] * (grad - unit_rows * proj)).astype(jnp.bfloat16)

        part[...] = lax.dot_general(feats[arr][...], embs[arr][...], CONTRACT_ROWS, preferred_element_type=jnp.float32)

    def tile_copy(u):
        arr, (slot, half) = u // N_TILES, ORDER[u % N_TILES]
        return pltpu.make_async_copy(gat.at[arr, slot, rows_of(half)], tiles.at[u % 4], tile_sem.at[u % 4])

    def comm(u):
        if u + 1 < 2 * N_TILES:
            arr, (slot, half) = (u + 1) // N_TILES, ORDER[(u + 1) % N_TILES]
            arrived(arr, slot, half)
            tile_copy(u + 1).start()
            if (arr, slot, half) == (0, 12, 1):
                for h in range(2):
                    send_own(1, h)
        if u in REDUCE_STEPS:
            reduce_phase(0, REDUCE_STEPS[u])
        if u < 2 * N_TILES:
            tile_copy(u).wait()
        if u >= 1:
            v = u - 1
            slot, half = ORDER[v % N_TILES]
            if v < N_TILES and half == 0 and slot:
                ids_copy(slot).wait_recv()
            src = ids_row if slot == 0 else ids_all.at[slot]
            ids_cur[...] = src[:, half * TILE:(half + 1) * TILE]

    def step(par, d1_arr, vpu_arr, d2_arr, cur_buf, old_buf):
        mxu, vpu = [], []
        if d1_arr is not None:
            mxu += d1_pieces((emb_img, emb_txt)[d1_arr], tiles.at[cur_buf], sims[par])
        if d2_arr is not None:
            mxu += d2_pieces(grads[par], tiles.at[old_buf], (acc_img, acc_txt)[d2_arr])
        if vpu_arr is not None:
            vpu = vpu_pieces(vpu_arr == 0, neg_scale, neg_bias, sims[1 - par], grads[1 - par],
                             ids_own, ids_cur, sums)
        interleave(mxu, vpu)

    load(0, 0).start()
    load(0, 1).start()
    load(1, 0).start()
    barrier = pltpu.get_barrier_semaphore()
    for slot in range(1, SLOTS):
        pl.semaphore_signal(barrier, inc=1, device_id=(xor_dev(slot),), device_id_type=MESH_ID)
    load(0, 0).wait()
    load(0, 1).wait()
    embed_half(0, 0)
    pl.semaphore_wait(barrier, SLOTS - 1)
    own_copy(0, 0).wait()
    send_own(0, 0)
    tile_copy(0).start()
    for slot in range(1, SLOTS):
        ids_copy(slot).start()
    embed_half(0, 1)
    load(1, 1).start()
    own_copy(0, 1).wait()
    send_own(0, 1)
    unit_out = pltpu.make_async_copy(unit, unit_hbm, unit_sem.at[0])
    unit_out.start()
    for block in range(0, ROWS, 128):
        ids_own[block:block + 128, :] = ids_column(ids_row[:, block:block + 128])
    acc_img[...] = jnp.zeros_like(acc_img)
    acc_txt[...] = jnp.zeros_like(acc_txt)
    for out in sums:
        out[...] = jnp.zeros(out.shape, jnp.float32)
    load(1, 0).wait()
    load(1, 1).wait()
    unit_out.wait()
    for half in range(2):
        embed_half(1, half)
    for half in range(2):
        own_copy(1, half).wait()

    comm(0)
    step(0, 0, None, None, 0, 0)
    comm(1)
    step(1, 0, 0, None, 1, 0)

    def run_loop(arr, start):
        n_iter = (N_TILES - 2) // 2

        @pl.loop(0, n_iter)
        def _(it):
            base = (start // 2) % 2
            buf = 2 * lax.rem(it + base, 2)
            for par in range(2):
                for k in range(n_iter):
                    pl.when(it == k)(functools.partial(comm, start + 2 * k + par))
                step(par, arr, arr, arr, buf + par, (2 - buf) + par)

    run_loop(0, 2)
    comm(N_TILES)
    step(0, 1, 0, 0, N_TILES % 4, (N_TILES - 2) % 4)
    for slot in range(1, SLOTS):
        sums_copy(slot).start()
    comm(N_TILES + 1)
    step(1, 1, 1, 0, (N_TILES + 1) % 4, (N_TILES - 1) % 4)
    finish(1, acc_img)
    reduce_phase(0, 0)
    unit_in = pltpu.make_async_copy(unit_hbm, unit, unit_sem.at[1])
    unit_in.start()
    run_loop(1, N_TILES + 2)
    comm(2 * N_TILES)
    step(0, None, 1, 1, 0, (2 * N_TILES - 2) % 4)
    step(1, None, None, 1, 0, (2 * N_TILES - 1) % 4)
    reduce_phase(0, 8)
    unit_in.wait()
    finish(0, acc_txt)
    reduce_phase(1, 0)

    for slot in range(1, SLOTS):
        sums_copy(slot).wait_recv()
    for i in range(3):
        parts = [sums_all[slot, i] for slot in range(SLOTS)]
        while len(parts) > 1:
            parts = [parts[j] + parts[j + 1] for j in range(0, len(parts), 2)]
        totals[i] = parts[0]
    for phase in range(1, 9):
        reduce_phase(1, phase)

    for slot in range(1, SLOTS):
        ids_copy(slot).wait_send()
        sums_copy(slot).wait_send()
    for arr in range(2):
        for half in range(2):
            for color in range(3):
                for i in range(7):
                    transfer(arr, half, color, i).wait_send()
            for slot in range(0, SLOTS, 2):
                pair_copy(arr, half, slot).wait_send()


def main_call(scal, feat_txt, feat_img, w_txt, w_img, ids):
    vmem = pl.BlockSpec(memory_space=pltpu.VMEM)
    hbm = pl.BlockSpec(memory_space=pl.ANY)
    f32, bf16 = jnp.float32, jnp.bfloat16
    dma = pltpu.SemaphoreType.DMA
    return pl.pallas_call(
        main_kernel,
        in_specs=[pl.BlockSpec(memory_space=pltpu.SMEM)] + [hbm] * 4 + [vmem],
        out_specs=[vmem] * 3 + [hbm] * 2,
        out_shape=[jax.ShapeDtypeStruct((DIM, DIM), f32)] * 2 + [jax.ShapeDtypeStruct((3, 8, 128), f32)]
        + [jax.ShapeDtypeStruct((2, SLOTS, ROWS, DIM), bf16), jax.ShapeDtypeStruct((ROWS, DIM), f32)],
        scratch_shapes=[
            pltpu.VMEM((ROWS, 128), jnp.int32),
            pltpu.VMEM((ROWS, DIM), bf16), pltpu.VMEM((ROWS, DIM), bf16),
            pltpu.VMEM((DIM, DIM), bf16), pltpu.VMEM((DIM, DIM), f32),
            pltpu.VMEM((ROWS, DIM), f32), pltpu.VMEM((ROWS, 1), f32), pltpu.VMEM((ROWS, 1), f32),
            pltpu.VMEM((ROWS, DIM), bf16), pltpu.VMEM((ROWS, DIM), bf16),
            pltpu.VMEM((ROWS, DIM), f32), pltpu.VMEM((ROWS, DIM), f32),
            pltpu.VMEM((4, TILE, DIM), bf16),
            pltpu.VMEM((ROWS, TILE), f32), pltpu.VMEM((ROWS, TILE), f32),
            pltpu.VMEM((ROWS, TILE), bf16), pltpu.VMEM((ROWS, TILE), bf16),
            pltpu.VMEM((SLOTS, 1, ROWS), jnp.int32), pltpu.VMEM((1, TILE), jnp.int32),
            pltpu.VMEM((SLOTS, 3, 8, 128), f32), pltpu.VMEM((HALF_DIM, DIM), f32),
            pltpu.VMEM((3, RS_ROWS[0], COLOR), f32), pltpu.VMEM((3, RS_ROWS[1], COLOR), f32),
            pltpu.VMEM((3, RS_ROWS[2], COLOR), f32),
            dma((2, 2, 3, 7)), dma((2, 2, 3, 7)), dma((2, 2, 8)), dma((2, 2, 8)), dma((SLOTS,)), dma((SLOTS,)),
            dma((4,)), dma((2, 2)), dma((2,)), dma((2, 2)), dma((SLOTS,)), dma((SLOTS,)),
            dma((2, 2)), dma((2, 2)), dma((2, 3, 6)), dma((2, 3, 6)),
        ],
        compiler_params=pltpu.CompilerParams(collective_id=0, has_side_effects=True, vmem_limit_bytes=67043328),
    )(scal, feat_txt, feat_img, w_txt, w_img, ids[None, :])


def solution(mesh):
    n_dev = mesh.shape["data"]

    def local_fn(feat_img, feat_txt, w_img, w_txt, log_temp, logit_bias, pair_ids):
        total_rows = feat_img.shape[0] * n_dev
        temp_scale = jnp.exp(log_temp)
        scal = jnp.stack([-temp_scale * LOG2E, -logit_bias * LOG2E, temp_scale / total_rows])
        dw_img, dw_txt, totals = main_call(scal, feat_txt, feat_img, w_txt, w_img, pair_ids)[:3]
        sums = jnp.sum(totals, axis=(1, 2))
        return (sums[0] / (LOG2E * total_rows), temp_scale * sums[1] / total_rows, sums[2] / total_rows, dw_img, dw_txt)

    return jax.shard_map(
        local_fn,
        mesh=mesh,
        in_specs=(P("data", None), P("data", None), P(None, None), P(None, None), P(), P(), P("data")),
        out_specs=(P(), P(), P(), P(None, None), P(None, None)),
        check_vma=False,
    )
```

```python
import functools

import jax
import jax.numpy as jnp
from jax import lax
from jax.experimental import pallas as pl
from jax.experimental.pallas import tpu as pltpu
from jax.sharding import PartitionSpec as P

CONTRACT_ROWS = (((0,), (0,)), ((), ()))
CONTRACT_COLS = (((1,), (1,)), ((), ()))
LOG2E = 1.4426950408889634
MESH_ID = pl.DeviceIdType.MESH

ROWS, DIM = 1024, 1152
TILE = 512
COLOR = DIM // 3
LINK_BITS = (2, 4, 8)
SLOTS = 16
ROW_PIECE = 128
D1_PIECE = (256, 512)
D2_PIECE = (512, 512)
HALF_DIM = DIM // 2
RS_ROWS = (HALF_DIM // 2, HALF_DIM // 4, HALF_DIM // 8)
REDUCE_STEPS = {54: 1, 57: 2, 59: 3, 60: 4, 61: 5, 62: 6, 64: 7}


def transfer_table(color):
    b0, b1, b2 = (LINK_BITS[(color + j) % 3] for j in range(3))
    return ((b0, 0), (b1, 0), (b1, b0), (b2, 0), (b2, b0), (b2, b1), (b2, b0 | b1))


def tile_order():
    order = [(0, 0), (1, 0), (0, 1), (1, 1)]
    groups = [((2, 4, 8), 0), ((2, 4, 8), 1), ((6, 10, 12), 0), ((6, 10, 12), 1), ((14,), 0), ((14,), 1)]
    for slots, half in groups:
        for slot in slots:
            order += [(slot, half), (slot | 1, half)]
    return order


ORDER = tile_order()
N_TILES = len(ORDER)


def interleave(first, second):
    i = j = 0
    while i < len(first) or j < len(second):
        if j >= len(second) or (i < len(first) and i * len(second) <= j * len(first)):
            first[i]()
            i += 1
        else:
            second[j]()
            j += 1


def d1_pieces(own, tile, sim_out):
    def piece(m, n):
        sim_out[m:m + D1_PIECE[0], n:n + D1_PIECE[1]] = lax.dot_general(
            own[m:m + D1_PIECE[0], :], tile[n:n + D1_PIECE[1], :], CONTRACT_COLS, preferred_element_type=jnp.float32)

    return [functools.partial(piece, m, n) for n in range(0, TILE, D1_PIECE[1]) for m in range(0, ROWS, D1_PIECE[0])]


def d2_pieces(grad, tile, acc):
    def piece(m, n, end):
        acc[m:m + D2_PIECE[0], n:end] += jnp.dot(
            grad[m:m + D2_PIECE[0], :], tile[:, n:end], preferred_element_type=jnp.float32)

    return [functools.partial(piece, m, n, min(n + D2_PIECE[1], DIM))
            for m in range(0, ROWS, D2_PIECE[0]) for n in range(0, DIM, D2_PIECE[1])]


def vpu_pieces(want, neg_scale, neg_bias, sim, grad_out, ids_own, ids_rem, sums):
    state = {"terms": 0}

    def add(name, value):
        state[name] = state[name] + value if name in state else value

    def chunk(r0, c0):
        rows, cols = slice(r0, r0 + ROW_PIECE), slice(c0, c0 + 128)
        s = sim[rows, cols]
        neg_y = jnp.where(ids_own[rows, :] == ids_rem[:, cols], -1.0, 1.0)
        yz = (s * neg_scale + neg_bias) * neg_y
        if want:
            e = jnp.exp2(-jnp.abs(yz))
            r = 1.0 / (1.0 + e)
            grad = jnp.where(yz <= 0, r, e * r) * neg_y
            low = jnp.minimum(yz, 0.0)
            gs = grad * s
            while e.shape[0] > 8:
                mid = e.shape[0] // 2
                e = e[:mid] + (e[mid:] + e[:mid] * e[mid:])
            state["prod"] = state["prod"] + (e + state["prod"] * e) if "prod" in state else e
            state["terms"] += ROW_PIECE // 8
            add("low", jnp.sum(low.reshape(-1, 8, 128), axis=0))
            add("gs", jnp.sum(gs.reshape(-1, 8, 128), axis=0))
            add("g", jnp.sum(grad.reshape(-1, 8, 128), axis=0))
            if state["terms"] == 64:
                state["low"] = state["low"] - jnp.log1p(state.pop("prod")) * LOG2E
                state["terms"] = 0
        else:
            grad = neg_y / (1.0 + jnp.exp2(yz))
        grad_out[rows, cols] = grad.astype(jnp.bfloat16)

    def piece(r0):
        for c0 in range(0, TILE, 128):
            chunk(r0, c0)
        if want and r0 + ROW_PIECE == ROWS:
            sums[0][...] -= state["low"]
            sums[1][...] += state["gs"]
            sums[2][...] += state["g"]

    return [functools.partial(piece, r0) for r0 in range(0, ROWS, ROW_PIECE)]


def ids_column(row):
    shape = (128, 128)
    diagonal = lax.broadcasted_iota(jnp.int32, shape, 0) == lax.broadcasted_iota(jnp.int32, shape, 1)
    picked = jnp.where(diagonal, jnp.broadcast_to(row.astype(jnp.float32), shape), 0.0)
    return jnp.broadcast_to(jnp.sum(picked, axis=1, keepdims=True), shape).astype(jnp.int32)


def main_kernel(scal, feat_txt, feat_img, w_txt, w_img, ids_row,
                dw_img, dw_txt, totals, gat, unit_hbm,
                ids_own, feat0, feat1, wgt, part, unit, inv0, inv1, emb_txt, emb_img, acc_img, acc_txt,
                tiles, sim0, sim1, grad0, grad1, ids_all, ids_cur, sums_all, rx_pair, rx1, rx2, rx3,
                send_sem, recv_sem, pair_send, pair_recv, ids_send, ids_recv, tile_sem, load_sem, unit_sem, own_sem,
                sum_send, sum_recv, half_send, half_recv, ring_send, ring_recv):
    me = lax.axis_index("data")
    embs = (emb_txt, emb_img)
    feats, invs = (feat0, feat1), (inv0, inv1)
    sims, grads = (sim0, sim1), (grad0, grad1)
    sums = tuple(sums_all.at[0, i] for i in range(3))
    neg_scale, neg_bias, factor = scal[0], scal[1], scal[2]

    def bit_of(bit):
        return lax.rem(lax.div(me, bit), 2)

    peer = {bit: me + bit * (1 - 2 * bit_of(bit)) for bit in (1, 2, 4, 8)}

    def xor_dev(slot):
        dev = me
        for bit in (1, 2, 4, 8):
            if slot & bit:
                dev = dev + (peer[bit] - me)
        return dev

    def remote(src, dst, send, recv, dev):
        return pltpu.make_async_remote_copy(src_ref=src, dst_ref=dst, send_sem=send, recv_sem=recv,
                                            device_id=(dev,), device_id_type=MESH_ID)

    def rows_of(half):
        return pl.ds(half * TILE if isinstance(half, int) else pl.multiple_of(half * TILE, TILE), TILE)

    def transfer(arr, half, color, i):
        link, slot = transfer_table(color)[i]
        cols = pl.ds(color * COLOR, COLOR)
        return remote(gat.at[arr, slot, rows_of(half), cols], gat.at[arr, slot | link, rows_of(half), cols],
                      send_sem.at[arr, half, color, i], recv_sem.at[arr, half, color, i], peer[link])

    def pair_copy(arr, half, slot):
        return remote(gat.at[arr, slot, rows_of(half)], gat.at[arr, slot | 1, rows_of(half)],
                      pair_send.at[arr, half, slot // 2], pair_recv.at[arr, half, slot // 2], peer[1])

    def ids_copy(slot):
        return remote(ids_row, ids_all.at[slot], ids_send.at[slot], ids_recv.at[slot], xor_dev(slot))

    def sums_copy(slot):
        return remote(sums_all.at[0], sums_all.at[slot], sum_send.at[slot], sum_recv.at[slot], xor_dev(slot))

    def send_own(arr, half):
        pair_copy(arr, half, 0).start()
        for j in range(3):
            for d in range(3):
                color = (d - j) % 3
                transfer(arr, half, color, (0, 1, 3)[j]).start()

    def arrived(arr, slot, half):
        if slot == 0:
            return
        if slot & 1:
            pair_copy(arr, half, slot - 1).wait_recv()
            return
        for color in range(3):
            for i, (link, src) in enumerate(transfer_table(color)):
                if src | link == slot:
                    transfer(arr, half, color, i).wait_recv()
        for color in range(3):
            for i, (link, src) in enumerate(transfer_table(color)):
                if src == slot:
                    transfer(arr, half, color, i).start()
        pair_copy(arr, half, slot).start()

    dws = (dw_img, dw_txt)
    rxs = (rx1, rx2, rx3)

    def half_copy(arr, last):
        core = bit_of(1)
        start = HALF_DIM * (core if last else 1 - core)
        src = (dws[arr] if last else part).at[pl.ds(pl.multiple_of(start, 8), HALF_DIM)]
        return remote(src, src if last else rx_pair, half_send.at[arr, last], half_recv.at[arr, last], peer[1])

    def ring_offset(color, depth, flip_last):
        off = HALF_DIM * bit_of(1)
        for j in range(depth):
            bit = bit_of(LINK_BITS[(color + j) % 3])
            if flip_last and j == depth - 1:
                bit = 1 - bit
            off = off + RS_ROWS[j] * bit
        return pl.multiple_of(off, 8)

    def ring_copy(arr, color, phase):
        cols = pl.ds(color * COLOR, COLOR)
        if phase < 3:
            rows = pl.ds(ring_offset(color, phase + 1, True), RS_ROWS[phase])
            src, dst, dim = part.at[rows, cols], rxs[phase].at[color], phase
        else:
            dim = 5 - phase
            rows = pl.ds(ring_offset(color, dim + 1, False), RS_ROWS[dim])
            src = dst = dws[arr].at[rows, cols]
        return remote(src, dst, ring_send.at[arr, color, phase], ring_recv.at[arr, color, phase],
                      peer[LINK_BITS[(color + dim) % 3]])

    def reduce_phase(arr, phase):
        if phase == 0:
            half_copy(arr, 0).start()
            return
        if phase == 1:
            half_copy(arr, 0).wait_recv()
            base = HALF_DIM * bit_of(1)

            @pl.loop(0, HALF_DIM // 32)
            def _(i):
                rows = pl.ds(pl.multiple_of(base + i * 32, 8), 32)
                part[rows, :] += rx_pair[pl.ds(pl.multiple_of(i * 32, 8), 32), :]

            for color in range(3):
                ring_copy(arr, color, 0).start()
            return
        if phase <= 4:
            done = phase - 2
            n_rows = RS_ROWS[done]
            for color in range(3):
                ring_copy(arr, color, done).wait_recv()
                cols = pl.ds(color * COLOR, COLOR)
                base = ring_offset(color, done + 1, False)

                @pl.loop(0, n_rows // 24)
                def _(i):
                    rows = pl.ds(pl.multiple_of(base + i * 24, 8), 24)
                    total = part[rows, cols] + rxs[done][color, pl.ds(pl.multiple_of(i * 24, 8), 24), :]
                    (dws[arr] if done == 2 else part)[rows, cols] = total

                ring_copy(arr, color, done + 1).start()
            return
        if phase <= 6:
            for color in range(3):
                ring_copy(arr, color, phase - 2).wait_recv()
                ring_copy(arr, color, phase - 1).start()
            return
        if phase == 7:
            for color in range(3):
                ring_copy(arr, color, 5).wait_recv()
            half_copy(arr, 1).start()
            return
        half_copy(arr, 1).wait_recv()
        for last in range(2):
            half_copy(arr, last).wait_send()
        for color in range(3):
            for ph in range(6):
                ring_copy(arr, color, ph).wait_send()

    def load(arr, which):
        src, dst = (((feat_txt, feat0), (w_txt, wgt)), ((feat_img, feat1), (w_img, wgt)))[arr][which]
        return pltpu.make_async_copy(src, dst, load_sem.at[arr, which])

    def own_copy(arr, half):
        return pltpu.make_async_copy(embs[arr].at[rows_of(half)], gat.at[arr, 0, rows_of(half)], own_sem.at[arr, half])

    def embed_half(arr, half):
        rows = rows_of(half)
        raw = jnp.dot(feats[arr][rows, :], wgt[...], preferred_element_type=jnp.float32)
        inv = lax.rsqrt(jnp.sum(raw * raw, axis=1, keepdims=True))
        unit_rows = raw * inv
        unit[rows, :] = unit_rows
        invs[arr][rows, :] = inv
        embs[arr][rows, :] = unit_rows.astype(jnp.bfloat16)
        own_copy(arr, half).start()

    def finish(arr, acc):
        @pl.loop(0, ROWS // 64)
        def _(i):
            rows = pl.ds(pl.multiple_of(i * 64, 64), 64)
            grad = factor * acc[rows, :]
            unit_rows = unit[rows, :]
            proj = jnp.sum(unit_rows * grad, axis=1, keepdims=True)
            embs[arr][rows, :] = (invs[arr][rows, :] * (grad - unit_rows * proj)).astype(jnp.bfloat16)

        part[...] = lax.dot_general(feats[arr][...], embs[arr][...], CONTRACT_ROWS, preferred_element_type=jnp.float32)

    def tile_copy(u):
        arr, (slot, half) = u // N_TILES, ORDER[u % N_TILES]
        return pltpu.make_async_copy(gat.at[arr, slot, rows_of(half)], tiles.at[u % 4], tile_sem.at[u % 4])

    def comm(u):
        if u + 1 < 2 * N_TILES:
            arr, (slot, half) = (u + 1) // N_TILES, ORDER[(u + 1) % N_TILES]
            arrived(arr, slot, half)
            tile_copy(u + 1).start()
            if (arr, slot, half) == (0, 12, 1):
                for h in range(2):
                    send_own(1, h)
        if u in REDUCE_STEPS:
            reduce_phase(0, REDUCE_STEPS[u])
        if u < 2 * N_TILES:
            tile_copy(u).wait()
        if u >= 1:
            v = u - 1
            slot, half = ORDER[v % N_TILES]
            if v < N_TILES and half == 0 and slot:
                ids_copy(slot).wait_recv()
            src = ids_row if slot == 0 else ids_all.at[slot]
            ids_cur[...] = src[:, half * TILE:(half + 1) * TILE]

    def step(par, d1_arr, vpu_arr, d2_arr, cur_buf, old_buf):
        mxu, vpu = [], []
        if d1_arr is not None:
            mxu += d1_pieces((emb_img, emb_txt)[d1_arr], tiles.at[cur_buf], sims[par])
        if d2_arr is not None:
            mxu += d2_pieces(grads[par], tiles.at[old_buf], (acc_img, acc_txt)[d2_arr])
        if vpu_arr is not None:
            vpu = vpu_pieces(vpu_arr == 0, neg_scale, neg_bias, sims[1 - par], grads[1 - par],
                             ids_own, ids_cur, sums)
        interleave(mxu, vpu)

    load(0, 0).start()
    load(0, 1).start()
    load(1, 0).start()
    barrier = pltpu.get_barrier_semaphore()
    for slot in range(1, SLOTS):
        pl.semaphore_signal(barrier, inc=1, device_id=(xor_dev(slot),), device_id_type=MESH_ID)
    load(0, 0).wait()
    load(0, 1).wait()
    embed_half(0, 0)
    pl.semaphore_wait(barrier, SLOTS - 1)
    own_copy(0, 0).wait()
    send_own(0, 0)
    tile_copy(0).start()
    for slot in range(1, SLOTS):
        ids_copy(slot).start()
    embed_half(0, 1)
    load(1, 1).start()
    own_copy(0, 1).wait()
    send_own(0, 1)
    unit_out = pltpu.make_async_copy(unit, unit_hbm, unit_sem.at[0])
    unit_out.start()
    for block in range(0, ROWS, 128):
        ids_own[block:block + 128, :] = ids_column(ids_row[:, block:block + 128])
    acc_img[...] = jnp.zeros_like(acc_img)
    acc_txt[...] = jnp.zeros_like(acc_txt)
    for out in sums:
        out[...] = jnp.zeros(out.shape, jnp.float32)
    load(1, 0).wait()
    load(1, 1).wait()
    unit_out.wait()

    @pl.loop(0, 2)
    def _(half):
        embed_half(1, half)

    for half in range(2):
        own_copy(1, half).wait()

    comm(0)
    step(0, 0, None, None, 0, 0)
    comm(1)
    step(1, 0, 0, None, 1, 0)

    def run_loop(arr, start):
        n_iter = (N_TILES - 2) // 2

        @pl.loop(0, n_iter)
        def _(it):
            base = (start // 2) % 2
            buf = 2 * lax.rem(it + base, 2)
            for par in range(2):
                for k in range(n_iter):
                    pl.when(it == k)(functools.partial(comm, start + 2 * k + par))
                step(par, arr, arr, arr, buf + par, (2 - buf) + par)

    run_loop(0, 2)
    comm(N_TILES)
    step(0, 1, 0, 0, N_TILES % 4, (N_TILES - 2) % 4)
    for slot in range(1, SLOTS):
        sums_copy(slot).start()
    comm(N_TILES + 1)
    step(1, 1, 1, 0, (N_TILES + 1) % 4, (N_TILES - 1) % 4)
    finish(1, acc_img)
    reduce_phase(0, 0)
    unit_in = pltpu.make_async_copy(unit_hbm, unit, unit_sem.at[1])
    unit_in.start()
    run_loop(1, N_TILES + 2)
    comm(2 * N_TILES)
    step(0, None, 1, 1, 0, (2 * N_TILES - 2) % 4)
    step(1, None, None, 1, 0, (2 * N_TILES - 1) % 4)
    reduce_phase(0, 8)
    unit_in.wait()
    finish(0, acc_txt)
    reduce_phase(1, 0)

    for slot in range(1, SLOTS):
        sums_copy(slot).wait_recv()
    for i in range(3):
        parts = [sums_all[slot, i] for slot in range(SLOTS)]
        while len(parts) > 1:
            parts = [parts[j] + parts[j + 1] for j in range(0, len(parts), 2)]
        totals[i] = parts[0]
    for phase in range(1, 9):
        reduce_phase(1, phase)

    for slot in range(1, SLOTS):
        ids_copy(slot).wait_send()
        sums_copy(slot).wait_send()
    for arr in range(2):
        for half in range(2):
            for color in range(3):
                for i in range(7):
                    transfer(arr, half, color, i).wait_send()
            for slot in range(0, SLOTS, 2):
                pair_copy(arr, half, slot).wait_send()


def main_call(scal, feat_txt, feat_img, w_txt, w_img, ids):
    vmem = pl.BlockSpec(memory_space=pltpu.VMEM)
    hbm = pl.BlockSpec(memory_space=pl.ANY)
    f32, bf16 = jnp.float32, jnp.bfloat16
    dma = pltpu.SemaphoreType.DMA
    return pl.pallas_call(
        main_kernel,
        in_specs=[pl.BlockSpec(memory_space=pltpu.SMEM)] + [hbm] * 4 + [vmem],
        out_specs=[vmem] * 3 + [hbm] * 2,
        out_shape=[jax.ShapeDtypeStruct((DIM, DIM), f32)] * 2 + [jax.ShapeDtypeStruct((3, 8, 128), f32)]
        + [jax.ShapeDtypeStruct((2, SLOTS, ROWS, DIM), bf16), jax.ShapeDtypeStruct((ROWS, DIM), f32)],
        scratch_shapes=[
            pltpu.VMEM((ROWS, 128), jnp.int32),
            pltpu.VMEM((ROWS, DIM), bf16), pltpu.VMEM((ROWS, DIM), bf16),
            pltpu.VMEM((DIM, DIM), bf16), pltpu.VMEM((DIM, DIM), f32),
            pltpu.VMEM((ROWS, DIM), f32), pltpu.VMEM((ROWS, 1), f32), pltpu.VMEM((ROWS, 1), f32),
            pltpu.VMEM((ROWS, DIM), bf16), pltpu.VMEM((ROWS, DIM), bf16),
            pltpu.VMEM((ROWS, DIM), f32), pltpu.VMEM((ROWS, DIM), f32),
            pltpu.VMEM((4, TILE, DIM), bf16),
            pltpu.VMEM((ROWS, TILE), f32), pltpu.VMEM((ROWS, TILE), f32),
            pltpu.VMEM((ROWS, TILE), bf16), pltpu.VMEM((ROWS, TILE), bf16),
            pltpu.VMEM((SLOTS, 1, ROWS), jnp.int32), pltpu.VMEM((1, TILE), jnp.int32),
            pltpu.VMEM((SLOTS, 3, 8, 128), f32), pltpu.VMEM((HALF_DIM, DIM), f32),
            pltpu.VMEM((3, RS_ROWS[0], COLOR), f32), pltpu.VMEM((3, RS_ROWS[1], COLOR), f32),
            pltpu.VMEM((3, RS_ROWS[2], COLOR), f32),
            dma((2, 2, 3, 7)), dma((2, 2, 3, 7)), dma((2, 2, 8)), dma((2, 2, 8)), dma((SLOTS,)), dma((SLOTS,)),
            dma((4,)), dma((2, 2)), dma((2,)), dma((2, 2)), dma((SLOTS,)), dma((SLOTS,)),
            dma((2, 2)), dma((2, 2)), dma((2, 3, 6)), dma((2, 3, 6)),
        ],
        compiler_params=pltpu.CompilerParams(collective_id=0, has_side_effects=True, vmem_limit_bytes=67043328),
    )(scal, feat_txt, feat_img, w_txt, w_img, ids[None, :])


def solution(mesh):
    n_dev = mesh.shape["data"]

    def local_fn(feat_img, feat_txt, w_img, w_txt, log_temp, logit_bias, pair_ids):
        total_rows = feat_img.shape[0] * n_dev
        temp_scale = jnp.exp(log_temp)
        scal = jnp.stack([-temp_scale * LOG2E, -logit_bias * LOG2E, temp_scale / total_rows])
        dw_img, dw_txt, totals = main_call(scal, feat_txt, feat_img, w_txt, w_img, pair_ids)[:3]
        sums = jnp.sum(totals, axis=(1, 2))
        return (sums[0] / (LOG2E * total_rows), temp_scale * sums[1] / total_rows, sums[2] / total_rows, dw_img, dw_txt)

    return jax.shard_map(
        local_fn,
        mesh=mesh,
        in_specs=(P("data", None), P("data", None), P(None, None), P(None, None), P(), P(), P("data")),
        out_specs=(P(), P(), P(), P(None, None), P(None, None)),
        check_vma=False,
    )
```

```python
import functools

import jax
import jax.numpy as jnp
from jax import lax
from jax.experimental import pallas as pl
from jax.experimental.pallas import tpu as pltpu
from jax.sharding import PartitionSpec as P

CONTRACT_ROWS = (((0,), (0,)), ((), ()))
CONTRACT_COLS = (((1,), (1,)), ((), ()))
LOG2E = 1.4426950408889634
MESH_ID = pl.DeviceIdType.MESH

ROWS, DIM = 1024, 1152
TILE = 512
COLOR = DIM // 3
LINK_BITS = (2, 4, 8)
SLOTS = 16
ROW_PIECE = 128
D1_PIECE = (256, 512)
D2_PIECE = (512, 512)
HALF_DIM = DIM // 2
RS_ROWS = (HALF_DIM // 2, HALF_DIM // 4, HALF_DIM // 8)
REDUCE_STEPS = {54: 1, 57: 2, 59: 3, 60: 4, 61: 5, 62: 6, 64: 7}


def transfer_table(color):
    b0, b1, b2 = (LINK_BITS[(color + j) % 3] for j in range(3))
    return ((b0, 0), (b1, 0), (b1, b0), (b2, 0), (b2, b0), (b2, b1), (b2, b0 | b1))


def tile_order():
    order = [(0, 0), (1, 0), (0, 1), (1, 1)]
    groups = [((2, 4, 8), 0), ((2, 4, 8), 1), ((6, 10, 12), 0), ((6, 10, 12), 1), ((14,), 0), ((14,), 1)]
    for slots, half in groups:
        for slot in slots:
            order += [(slot, half), (slot | 1, half)]
    return order


ORDER = tile_order()
N_TILES = len(ORDER)


def interleave(first, second):
    i = j = 0
    while i < len(first) or j < len(second):
        if j >= len(second) or (i < len(first) and i * len(second) <= j * len(first)):
            first[i]()
            i += 1
        else:
            second[j]()
            j += 1


def d1_pieces(own, tile, sim_out):
    def piece(m, n):
        sim_out[m:m + D1_PIECE[0], n:n + D1_PIECE[1]] = lax.dot_general(
            own[m:m + D1_PIECE[0], :], tile[n:n + D1_PIECE[1], :], CONTRACT_COLS, preferred_element_type=jnp.float32)

    return [functools.partial(piece, m, n) for n in range(0, TILE, D1_PIECE[1]) for m in range(0, ROWS, D1_PIECE[0])]


def d2_pieces(grad, tile, acc):
    def piece(m, n, end):
        acc[m:m + D2_PIECE[0], n:end] += jnp.dot(
            grad[m:m + D2_PIECE[0], :], tile[:, n:end], preferred_element_type=jnp.float32)

    return [functools.partial(piece, m, n, min(n + D2_PIECE[1], DIM))
            for m in range(0, ROWS, D2_PIECE[0]) for n in range(0, DIM, D2_PIECE[1])]


def vpu_pieces(want, neg_scale, neg_bias, sim, grad_out, ids_own, ids_rem, sums):
    state = {"terms": 0}

    def add(name, value):
        state[name] = state[name] + value if name in state else value

    def chunk(r0, c0):
        rows, cols = slice(r0, r0 + ROW_PIECE), slice(c0, c0 + 128)
        s = sim[rows, cols]
        neg_y = jnp.where(ids_own[rows, :] == ids_rem[:, cols], -1.0, 1.0)
        yz = (s * neg_scale + neg_bias) * neg_y
        if want:
            e = jnp.exp2(-jnp.abs(yz))
            r = 1.0 / (1.0 + e)
            grad = jnp.where(yz <= 0, r, e * r) * neg_y
            low = jnp.minimum(yz, 0.0)
            gs = grad * s
            while e.shape[0] > 8:
                mid = e.shape[0] // 2
                e = e[:mid] + (e[mid:] + e[:mid] * e[mid:])
            state["prod"] = state["prod"] + (e + state["prod"] * e) if "prod" in state else e
            state["terms"] += ROW_PIECE // 8
            add("low", jnp.sum(low.reshape(-1, 8, 128), axis=0))
            add("gs", jnp.sum(gs.reshape(-1, 8, 128), axis=0))
            add("g", jnp.sum(grad.reshape(-1, 8, 128), axis=0))
            if state["terms"] == 64:
                state["low"] = state["low"] - jnp.log1p(state.pop("prod")) * LOG2E
                state["terms"] = 0
        else:
            grad = neg_y / (1.0 + jnp.exp2(yz))
        grad_out[rows, cols] = grad.astype(jnp.bfloat16)

    def piece(r0):
        for c0 in range(0, TILE, 128):
            chunk(r0, c0)
        if want and r0 + ROW_PIECE == ROWS:
            sums[0][...] -= state["low"]
            sums[1][...] += state["gs"]
            sums[2][...] += state["g"]

    return [functools.partial(piece, r0) for r0 in range(0, ROWS, ROW_PIECE)]


def ids_column(row):
    shape = (128, 128)
    diagonal = lax.broadcasted_iota(jnp.int32, shape, 0) == lax.broadcasted_iota(jnp.int32, shape, 1)
    picked = jnp.where(diagonal, jnp.broadcast_to(row.astype(jnp.float32), shape), 0.0)
    return jnp.broadcast_to(jnp.sum(picked, axis=1, keepdims=True), shape).astype(jnp.int32)


def main_kernel(scal, feat_txt, feat_img, w_txt, w_img, ids_row,
                dw_img, dw_txt, totals, gat, unit_hbm,
                ids_own, feat0, feat1, wgt, part, unit, inv0, inv1, emb_txt, emb_img, acc_img, acc_txt,
                tiles, sim0, sim1, grad0, grad1, ids_all, ids_cur, sums_all, rx_pair, rx1, rx2, rx3,
                send_sem, recv_sem, pair_send, pair_recv, ids_send, ids_recv, tile_sem, load_sem, unit_sem, own_sem,
                sum_send, sum_recv, half_send, half_recv, ring_send, ring_recv):
    me = lax.axis_index("data")
    embs = (emb_txt, emb_img)
    feats, invs = (feat0, feat1), (inv0, inv1)
    sims, grads = (sim0, sim1), (grad0, grad1)
    sums = tuple(sums_all.at[0, i] for i in range(3))
    neg_scale, neg_bias, factor = scal[0], scal[1], scal[2]

    def bit_of(bit):
        return lax.rem(lax.div(me, bit), 2)

    peer = {bit: me + bit * (1 - 2 * bit_of(bit)) for bit in (1, 2, 4, 8)}

    def xor_dev(slot):
        dev = me
        for bit in (1, 2, 4, 8):
            if slot & bit:
                dev = dev + (peer[bit] - me)
        return dev

    def remote(src, dst, send, recv, dev):
        return pltpu.make_async_remote_copy(src_ref=src, dst_ref=dst, send_sem=send, recv_sem=recv,
                                            device_id=(dev,), device_id_type=MESH_ID)

    def rows_of(half):
        return pl.ds(half * TILE if isinstance(half, int) else pl.multiple_of(half * TILE, TILE), TILE)

    def transfer(arr, half, color, i):
        link, slot = transfer_table(color)[i]
        cols = pl.ds(color * COLOR, COLOR)
        return remote(gat.at[arr, slot, rows_of(half), cols], gat.at[arr, slot | link, rows_of(half), cols],
                      send_sem.at[arr, half, color, i], recv_sem.at[arr, half, color, i], peer[link])

    def pair_copy(arr, half, slot):
        return remote(gat.at[arr, slot, rows_of(half)], gat.at[arr, slot | 1, rows_of(half)],
                      pair_send.at[arr, half, slot // 2], pair_recv.at[arr, half, slot // 2], peer[1])

    def ids_copy(slot):
        return remote(ids_row, ids_all.at[slot], ids_send.at[slot], ids_recv.at[slot], xor_dev(slot))

    def sums_copy(slot):
        return remote(sums_all.at[0], sums_all.at[slot], sum_send.at[slot], sum_recv.at[slot], xor_dev(slot))

    def send_own(arr, half):
        pair_copy(arr, half, 0).start()
        for j in range(3):
            for d in range(3):
                color = (d - j) % 3
                transfer(arr, half, color, (0, 1, 3)[j]).start()

    def arrived(arr, slot, half):
        if slot == 0:
            return
        if slot & 1:
            pair_copy(arr, half, slot - 1).wait_recv()
            return
        for color in range(3):
            for i, (link, src) in enumerate(transfer_table(color)):
                if src | link == slot:
                    transfer(arr, half, color, i).wait_recv()
        for color in range(3):
            for i, (link, src) in enumerate(transfer_table(color)):
                if src == slot:
                    transfer(arr, half, color, i).start()
        pair_copy(arr, half, slot).start()

    dws = (dw_img, dw_txt)
    rxs = (rx1, rx2, rx3)

    def half_copy(arr, last):
        core = bit_of(1)
        start = HALF_DIM * (core if last else 1 - core)
        src = (dws[arr] if last else part).at[pl.ds(pl.multiple_of(start, 8), HALF_DIM)]
        return remote(src, src if last else rx_pair, half_send.at[arr, last], half_recv.at[arr, last], peer[1])

    def ring_offset(color, depth, flip_last):
        off = HALF_DIM * bit_of(1)
        for j in range(depth):
            bit = bit_of(LINK_BITS[(color + j) % 3])
            if flip_last and j == depth - 1:
                bit = 1 - bit
            off = off + RS_ROWS[j] * bit
        return pl.multiple_of(off, 8)

    def ring_copy(arr, color, phase):
        cols = pl.ds(color * COLOR, COLOR)
        if phase < 3:
            rows = pl.ds(ring_offset(color, phase + 1, True), RS_ROWS[phase])
            src, dst, dim = part.at[rows, cols], rxs[phase].at[color], phase
        else:
            dim = 5 - phase
            rows = pl.ds(ring_offset(color, dim + 1, False), RS_ROWS[dim])
            src = dst = dws[arr].at[rows, cols]
        return remote(src, dst, ring_send.at[arr, color, phase], ring_recv.at[arr, color, phase],
                      peer[LINK_BITS[(color + dim) % 3]])

    def reduce_phase(arr, phase):
        if phase == 0:
            half_copy(arr, 0).start()
            return
        if phase == 1:
            half_copy(arr, 0).wait_recv()
            base = HALF_DIM * bit_of(1)

            @pl.loop(0, HALF_DIM // 32)
            def _(i):
                rows = pl.ds(pl.multiple_of(base + i * 32, 8), 32)
                part[rows, :] += rx_pair[pl.ds(pl.multiple_of(i * 32, 8), 32), :]

            for color in range(3):
                ring_copy(arr, color, 0).start()
            return
        if phase <= 4:
            done = phase - 2
            n_rows = RS_ROWS[done]
            for color in range(3):
                ring_copy(arr, color, done).wait_recv()
                cols = pl.ds(color * COLOR, COLOR)
                base = ring_offset(color, done + 1, False)

                @pl.loop(0, n_rows // 24)
                def _(i):
                    rows = pl.ds(pl.multiple_of(base + i * 24, 8), 24)
                    total = part[rows, cols] + rxs[done][color, pl.ds(pl.multiple_of(i * 24, 8), 24), :]
                    (dws[arr] if done == 2 else part)[rows, cols] = total

                ring_copy(arr, color, done + 1).start()
            return
        if phase <= 6:
            for color in range(3):
                ring_copy(arr, color, phase - 2).wait_recv()
                ring_copy(arr, color, phase - 1).start()
            return
        if phase == 7:
            for color in range(3):
                ring_copy(arr, color, 5).wait_recv()
            half_copy(arr, 1).start()
            return
        half_copy(arr, 1).wait_recv()
        for last in range(2):
            half_copy(arr, last).wait_send()
        for color in range(3):
            for ph in range(6):
                ring_copy(arr, color, ph).wait_send()

    def load(arr, which):
        src, dst = (((feat_txt, feat0), (w_txt, wgt)), ((feat_img, feat1), (w_img, wgt)))[arr][which]
        return pltpu.make_async_copy(src, dst, load_sem.at[arr, which])

    def own_copy(arr, half):
        return pltpu.make_async_copy(embs[arr].at[rows_of(half)], gat.at[arr, 0, rows_of(half)], own_sem.at[arr, half])

    def embed_half(arr, half):
        rows = rows_of(half)
        raw = jnp.dot(feats[arr][rows, :], wgt[...], preferred_element_type=jnp.float32)
        inv = lax.rsqrt(jnp.sum(raw * raw, axis=1, keepdims=True))
        unit_rows = raw * inv
        unit[rows, :] = unit_rows
        invs[arr][rows, :] = inv
        embs[arr][rows, :] = unit_rows.astype(jnp.bfloat16)
        own_copy(arr, half).start()

    def finish(arr, acc):
        @pl.loop(0, ROWS // 64)
        def _(i):
            rows = pl.ds(pl.multiple_of(i * 64, 64), 64)
            grad = factor * acc[rows, :]
            unit_rows = unit[rows, :]
            proj = jnp.sum(unit_rows * grad, axis=1, keepdims=True)
            embs[arr][rows, :] = (invs[arr][rows, :] * (grad - unit_rows * proj)).astype(jnp.bfloat16)

        part[...] = lax.dot_general(feats[arr][...], embs[arr][...], CONTRACT_ROWS, preferred_element_type=jnp.float32)

    def tile_copy(u):
        arr, (slot, half) = u // N_TILES, ORDER[u % N_TILES]
        return pltpu.make_async_copy(gat.at[arr, slot, rows_of(half)], tiles.at[u % 4], tile_sem.at[u % 4])

    def comm(u):
        if u + 1 < 2 * N_TILES:
            arr, (slot, half) = (u + 1) // N_TILES, ORDER[(u + 1) % N_TILES]
            arrived(arr, slot, half)
            tile_copy(u + 1).start()
            if (arr, slot, half) == (0, 12, 1):
                for h in range(2):
                    send_own(1, h)
        if u in REDUCE_STEPS:
            reduce_phase(0, REDUCE_STEPS[u])
        if u < 2 * N_TILES:
            tile_copy(u).wait()
        if u >= 1:
            v = u - 1
            slot, half = ORDER[v % N_TILES]
            if v < N_TILES and half == 0 and slot:
                ids_copy(slot).wait_recv()
            src = ids_row if slot == 0 else ids_all.at[slot]
            ids_cur[...] = src[:, half * TILE:(half + 1) * TILE]

    def step(par, d1_arr, vpu_arr, d2_arr, cur_buf, old_buf):
        mxu, vpu = [], []
        if d1_arr is not None:
            mxu += d1_pieces((emb_img, emb_txt)[d1_arr], tiles.at[cur_buf], sims[par])
        if d2_arr is not None:
            mxu += d2_pieces(grads[par], tiles.at[old_buf], (acc_img, acc_txt)[d2_arr])
        if vpu_arr is not None:
            vpu = vpu_pieces(vpu_arr == 0, neg_scale, neg_bias, sims[1 - par], grads[1 - par],
                             ids_own, ids_cur, sums)
        interleave(mxu, vpu)

    load(0, 0).start()
    load(0, 1).start()
    load(1, 0).start()
    barrier = pltpu.get_barrier_semaphore()
    for slot in range(1, SLOTS):
        pl.semaphore_signal(barrier, inc=1, device_id=(xor_dev(slot),), device_id_type=MESH_ID)
    load(0, 0).wait()
    load(0, 1).wait()
    embed_half(0, 0)
    pl.semaphore_wait(barrier, SLOTS - 1)
    own_copy(0, 0).wait()
    send_own(0, 0)
    tile_copy(0).start()
    for slot in range(1, SLOTS):
        ids_copy(slot).start()
    embed_half(0, 1)
    load(1, 1).start()
    own_copy(0, 1).wait()
    send_own(0, 1)
    unit_out = pltpu.make_async_copy(unit, unit_hbm, unit_sem.at[0])
    unit_out.start()
    for block in range(0, ROWS, 128):
        ids_own[block:block + 128, :] = ids_column(ids_row[:, block:block + 128])
    acc_img[...] = jnp.zeros_like(acc_img)
    acc_txt[...] = jnp.zeros_like(acc_txt)
    for out in sums:
        out[...] = jnp.zeros(out.shape, jnp.float32)
    load(1, 0).wait()
    load(1, 1).wait()
    unit_out.wait()

    @pl.loop(0, 2)
    def _(half):
        embed_half(1, half)

    for half in range(2):
        own_copy(1, half).wait()

    comm(0)
    step(0, 0, None, None, 0, 0)
    comm(1)
    step(1, 0, 0, None, 1, 0)

    def run_loop(arr, start):
        n_iter = (N_TILES - 2) // 2

        @pl.loop(0, n_iter)
        def _(it):
            base = (start // 2) % 2
            buf = 2 * lax.rem(it + base, 2)
            for par in range(2):
                for first in range(0, n_iter, 4):
                    @pl.when(lax.div(it, 4) == first // 4)
                    def _():
                        for k in range(first, min(first + 4, n_iter)):
                            pl.when(it == k)(functools.partial(comm, start + 2 * k + par))

                step(par, arr, arr, arr, buf + par, (2 - buf) + par)

    run_loop(0, 2)
    comm(N_TILES)
    step(0, 1, 0, 0, N_TILES % 4, (N_TILES - 2) % 4)
    for slot in range(1, SLOTS):
        sums_copy(slot).start()
    comm(N_TILES + 1)
    step(1, 1, 1, 0, (N_TILES + 1) % 4, (N_TILES - 1) % 4)
    finish(1, acc_img)
    reduce_phase(0, 0)
    unit_in = pltpu.make_async_copy(unit_hbm, unit, unit_sem.at[1])
    unit_in.start()
    run_loop(1, N_TILES + 2)
    comm(2 * N_TILES)
    step(0, None, 1, 1, 0, (2 * N_TILES - 2) % 4)
    step(1, None, None, 1, 0, (2 * N_TILES - 1) % 4)
    reduce_phase(0, 8)
    unit_in.wait()
    finish(0, acc_txt)
    reduce_phase(1, 0)

    for slot in range(1, SLOTS):
        sums_copy(slot).wait_recv()
    for i in range(3):
        parts = [sums_all[slot, i] for slot in range(SLOTS)]
        while len(parts) > 1:
            parts = [parts[j] + parts[j + 1] for j in range(0, len(parts), 2)]
        totals[i] = parts[0]
    for phase in range(1, 9):
        reduce_phase(1, phase)

    for slot in range(1, SLOTS):
        ids_copy(slot).wait_send()
        sums_copy(slot).wait_send()
    for arr in range(2):
        for half in range(2):
            for color in range(3):
                for i in range(7):
                    transfer(arr, half, color, i).wait_send()
            for slot in range(0, SLOTS, 2):
                pair_copy(arr, half, slot).wait_send()


def main_call(scal, feat_txt, feat_img, w_txt, w_img, ids):
    vmem = pl.BlockSpec(memory_space=pltpu.VMEM)
    hbm = pl.BlockSpec(memory_space=pl.ANY)
    f32, bf16 = jnp.float32, jnp.bfloat16
    dma = pltpu.SemaphoreType.DMA
    return pl.pallas_call(
        main_kernel,
        in_specs=[pl.BlockSpec(memory_space=pltpu.SMEM)] + [hbm] * 4 + [vmem],
        out_specs=[vmem] * 3 + [hbm] * 2,
        out_shape=[jax.ShapeDtypeStruct((DIM, DIM), f32)] * 2 + [jax.ShapeDtypeStruct((3, 8, 128), f32)]
        + [jax.ShapeDtypeStruct((2, SLOTS, ROWS, DIM), bf16), jax.ShapeDtypeStruct((ROWS, DIM), f32)],
        scratch_shapes=[
            pltpu.VMEM((ROWS, 128), jnp.int32),
            pltpu.VMEM((ROWS, DIM), bf16), pltpu.VMEM((ROWS, DIM), bf16),
            pltpu.VMEM((DIM, DIM), bf16), pltpu.VMEM((DIM, DIM), f32),
            pltpu.VMEM((ROWS, DIM), f32), pltpu.VMEM((ROWS, 1), f32), pltpu.VMEM((ROWS, 1), f32),
            pltpu.VMEM((ROWS, DIM), bf16), pltpu.VMEM((ROWS, DIM), bf16),
            pltpu.VMEM((ROWS, DIM), f32), pltpu.VMEM((ROWS, DIM), f32),
            pltpu.VMEM((4, TILE, DIM), bf16),
            pltpu.VMEM((ROWS, TILE), f32), pltpu.VMEM((ROWS, TILE), f32),
            pltpu.VMEM((ROWS, TILE), bf16), pltpu.VMEM((ROWS, TILE), bf16),
            pltpu.VMEM((SLOTS, 1, ROWS), jnp.int32), pltpu.VMEM((1, TILE), jnp.int32),
            pltpu.VMEM((SLOTS, 3, 8, 128), f32), pltpu.VMEM((HALF_DIM, DIM), f32),
            pltpu.VMEM((3, RS_ROWS[0], COLOR), f32), pltpu.VMEM((3, RS_ROWS[1], COLOR), f32),
            pltpu.VMEM((3, RS_ROWS[2], COLOR), f32),
            dma((2, 2, 3, 7)), dma((2, 2, 3, 7)), dma((2, 2, 8)), dma((2, 2, 8)), dma((SLOTS,)), dma((SLOTS,)),
            dma((4,)), dma((2, 2)), dma((2,)), dma((2, 2)), dma((SLOTS,)), dma((SLOTS,)),
            dma((2, 2)), dma((2, 2)), dma((2, 3, 6)), dma((2, 3, 6)),
        ],
        compiler_params=pltpu.CompilerParams(collective_id=0, has_side_effects=True, vmem_limit_bytes=67043328),
    )(scal, feat_txt, feat_img, w_txt, w_img, ids[None, :])


def solution(mesh):
    n_dev = mesh.shape["data"]

    def local_fn(feat_img, feat_txt, w_img, w_txt, log_temp, logit_bias, pair_ids):
        total_rows = feat_img.shape[0] * n_dev
        temp_scale = jnp.exp(log_temp)
        scal = jnp.stack([-temp_scale * LOG2E, -logit_bias * LOG2E, temp_scale / total_rows])
        dw_img, dw_txt, totals = main_call(scal, feat_txt, feat_img, w_txt, w_img, pair_ids)[:3]
        sums = jnp.sum(totals, axis=(1, 2))
        return (sums[0] / (LOG2E * total_rows), temp_scale * sums[1] / total_rows, sums[2] / total_rows, dw_img, dw_txt)

    return jax.shard_map(
        local_fn,
        mesh=mesh,
        in_specs=(P("data", None), P("data", None), P(None, None), P(None, None), P(), P(), P("data")),
        out_specs=(P(), P(), P(), P(None, None), P(None, None)),
        check_vma=False,
    )
```
